256 devices in a mesh: grp: 16 (over y_hi, x, core), shard: 16 (over z, y_lo).
Axes of the slice: x: 4, y: 4 (y_hi: 2, y_lo: 2; y = y_hi * 2 + y_lo), z: 8, core: 2. Of those that a mesh axis runs over, the one named last changes fastest.
Arguments:
- gradients: bfloat16 [16, 1024, 5120], P('grp', None, 'shard'), may hold values from -150 to 150
- left_factor: bfloat16 [16, 1024, 1024], P('grp'), may hold values from -1 to 2, as said below
- right_factor: bfloat16 [16, 5120, 5120], P('grp', 'shard'), may hold values from -1 to 2, as said below
Outputs:
- update: bfloat16 [16, 1024, 5120], P('grp', None, 'shard')
The draws below stay inside these ranges and needn't reach their ends.
Inputs may be any that keep to these rules, and one draw needn't show every extreme that they name: `left_factor`: each factor is upper triangular with a positive diagonal. `right_factor`: each factor is upper triangular with a positive diagonal.
All inputs are finite; a program needn't handle non-finite values.
Results may differ from the reference program's by a relative error of at most 0.0061.
Values may be sent and summed in bfloat16 or wider, within the bound.
A program may use at most 128 MiB of HBM per device.

```python
import math
import jax
import jax.numpy as jnp
from jax import lax

D = 5120
KV_WIDTH = 1024
WEIGHTS = 16


def triangular(key, count, width):
    keys = jax.random.split(jax.random.fold_in(key, 7), 2)
    diagonal = jax.random.uniform(keys[0], (count, width), minval=0.6, maxval=1.4)
    offdiag = jnp.clip(jax.random.normal(keys[1], (count, width, width)), -3.0, 3.0) * (0.7 / math.sqrt(width))
    upper = jnp.triu(offdiag, 1)
    return upper + diagonal[:, :, None] * jnp.eye(width, dtype=jnp.float32)[None]


def draw_left_factor(key, part):
    return triangular(jax.random.fold_in(key, 11), WEIGHTS, KV_WIDTH).astype(jnp.bfloat16)


def draw_right_factor(key, part):
    return triangular(jax.random.fold_in(key, 13), WEIGHTS, D).astype(jnp.bfloat16)


def draw_gradients(key, part):
    keys = jax.random.split(jax.random.fold_in(key, 17), 4)
    top = math.log(math.sqrt(10.0))
    row_scale = jnp.exp(jax.random.uniform(keys[0], (WEIGHTS, KV_WIDTH), minval=0.0, maxval=top))
    col_scale = jnp.exp(jax.random.uniform(keys[1], (WEIGHTS, D), minval=0.0, maxval=top))
    weight_scale = jnp.exp(jax.random.uniform(keys[2], (WEIGHTS,), minval=0.0, maxval=math.log(3.0)))
    base = jnp.clip(jax.random.normal(keys[3], (WEIGHTS, KV_WIDTH, D)), -5.0, 5.0)
    values = base * row_scale[:, :, None] * col_scale[:, None, :] * weight_scale[:, None, None]
    return values.astype(jnp.bfloat16)


def setup_inputs(seed: int = 0) -> dict:
    arg_keys = jax.random.split(jax.random.key(seed), 4)
    gradients = draw_gradients(jax.random.fold_in(arg_keys[3], 71), 0)
    left_factor = draw_left_factor(jax.random.fold_in(arg_keys[3], 71), 0)
    right_factor = draw_right_factor(jax.random.fold_in(arg_keys[3], 71), 0)
    return dict(gradients=gradients, left_factor=left_factor, right_factor=right_factor)


def precondition(items):
    gradient, left_q, right_q = items
    first = lax.dot_general(gradient, right_q, (((1,), (1,)), ((), ())), preferred_element_type=jnp.float32).astype(jnp.bfloat16)
    second = jnp.dot(first, right_q, preferred_element_type=jnp.float32).astype(jnp.bfloat16)
    third = jnp.dot(left_q, second, preferred_element_type=jnp.float32).astype(jnp.bfloat16)
    return lax.dot_general(left_q, third, (((0,), (0,)), ((), ())), preferred_element_type=jnp.float32)

def reference(gradients, left_factor, right_factor):
    precond = lax.map(precondition, (gradients, left_factor, right_factor))
    count = precond.shape[0] * precond.shape[1] * precond.shape[2]
    rms = jnp.sqrt(jnp.sum(precond * precond) / count + 1e-06)
    factor = jnp.minimum(jnp.float32(1.0), 1.1 / rms)
    return (precond * factor).astype(jnp.bfloat16)
```

```python
import functools

import jax
import jax.numpy as jnp
from jax import lax
from jax.experimental import pallas as pl
from jax.experimental.pallas import tpu as pltpu
from jax.sharding import Mesh
from jax.sharding import PartitionSpec as P

MESH = pl.DeviceIdType.MESH
SHARD = ("shard_0", "shard_1")
GRP = ("grp_0", "grp_1", "grp_2")
F32 = jnp.float32
BF16 = jnp.bfloat16

PLANES = 8
LANES = 128
HOPS = 4


def low(s):
    return jnp.where(s >= 4, 1, 0) + jnp.where(s >= 5, 1, 0) + jnp.where(s >= 7, 1, 0)


def single(s):
    return (s == 3) | (s >= 5)


def loop(lower, upper, body):
    def step(i, carry):
        body(i)
        return carry

    lax.fori_loop(lower, upper, step, 0)


def kernel(
    count,
    sizes,
    g_ref,
    qr_hbm,
    ql_hbm,
    out_ref,
    gt,
    buf,
    yin,
    qr,
    qrt,
    ql,
    first,
    second,
    precond,
    mine,
    all_shard,
    all_grp,
    down_send,
    up_send,
    cross_send,
    back_send,
    rcross_send,
    gz_recv,
    gy_recv,
    rz_recv,
    ry_recv,
    load_sem,
    ar_send,
    ar_recv,
):
    planes, chunks = PLANES, gt.shape[0]
    nb = g_ref.shape[1]
    z, y = lax.axis_index("shard_0"), lax.axis_index("shard_1")
    g0, g1, g2 = lax.axis_index("grp_0"), lax.axis_index("grp_1"), lax.axis_index("grp_2")
    n1, n2 = sizes[1], sizes[2]
    n_shard, n_grp = planes * 2, sizes[0] * n1 * n2
    shard_me = z * 2 + y
    grp_me = (g0 * n1 + g1) * n2 + g2
    up_z, down_z = lax.rem(z + 1, planes), lax.rem(z + planes - 1, planes)
    own = pl.ds(pl.multiple_of(y * nb, 16), nb)
    other = pl.ds(pl.multiple_of((1 - y) * nb, 16), nb)

    def shard_id(p):
        return {"shard_0": p // 2, "shard_1": lax.rem(p, 2)}

    def grp_id(p):
        return {"grp_0": p // (n1 * n2), "grp_1": lax.rem(p // n2, n1), "grp_2": lax.rem(p, n2)}

    def load(s):
        columns = pl.ds(pl.multiple_of(s * 2 * nb, 128), 2 * nb)
        return pltpu.make_async_copy(qr_hbm.at[:, columns], qr.at[s], load_sem.at[s])

    load_ql = pltpu.make_async_copy(ql_hbm, ql, load_sem.at[planes])
    loop(z, planes, lambda s: load(s).start())
    load_ql.start()

    barrier = pltpu.get_barrier_semaphore()

    def greet_shard(k):
        peer = lax.rem(shard_me + k, n_shard)
        pl.semaphore_signal(barrier, inc=1, device_id=shard_id(peer), device_id_type=MESH)

    def greet_grp(k):
        peer = lax.rem(grp_me + k, n_grp)
        pl.semaphore_signal(barrier, inc=1, device_id=grp_id(peer), device_id_type=MESH)

    loop(1, n_shard, greet_shard)
    loop(1, n_grp, greet_grp)

    def place(c):
        rows = pl.ds(pl.multiple_of(c * LANES, LANES), LANES)
        gt[c, z, own, :] = g_ref[rows, :].T

    loop(0, chunks, place)
    pl.semaphore_wait(barrier, n_shard + n_grp - 2)

    def remote(src, dst, send, recv, to_z, to_y):
        return pltpu.make_async_remote_copy(
            src_ref=src,
            dst_ref=dst,
            send_sem=send,
            recv_sem=recv,
            device_id={"shard_0": to_z, "shard_1": to_y},
            device_id_type=MESH,
        )

    def sized(s, act):
        pl.when(single(s))(lambda: act(own))
        pl.when(jnp.logical_not(single(s)))(lambda: act(pl.ds(0, 2 * nb)))

    def down(c, s, rows):
        ref = gt.at[c, s, rows]
        return remote(ref, ref, down_send.at[lax.rem(c, 2), s], gz_recv.at[c, s], down_z, y)

    def up(c, s, rows):
        ref = gt.at[c, s, rows]
        return remote(ref, ref, up_send.at[lax.rem(c, 2), s], gz_recv.at[c, s], up_z, y)

    def cross(c, s):
        ref = gt.at[c, s, own]
        return remote(ref, ref, cross_send.at[lax.rem(c, 2), s], gy_recv.at[c, s], z, 1 - y)

    def back(c, s, rows):
        rising = (z < s) & (z >= low(s))
        parent = jnp.where(rising, up_z, down_z)
        slot = jnp.where((parent == s) & jnp.logical_not(rising), planes, s)
        src = buf.at[jnp.where(z > s, 1, 0), c, s, rows]
        dst = buf.at[1, c, slot, rows]
        return remote(src, dst, back_send.at[lax.rem(c, 2), s], rz_recv.at[c, slot], parent, y)

    def rcross(c, s):
        return remote(
            buf.at[0, c, s, other], yin.at[c, s], rcross_send.at[lax.rem(c, 2), s], ry_recv.at[c, s], z, 1 - y
        )

    def goes_down(s):
        return (z <= s) & (z - 1 >= low(s))

    def goes_up(s):
        return ((z >= s) & (low(s) > 0)) | ((z < s) & (z + 1 < low(s)))

    def crosses(s):
        return (s == z) | ((s > z) & single(s))

    def goes_back(s):
        return (z < s) | ((z > s) & (low(s) > 0))

    def start(c, make):
        pl.when(c >= 2)(lambda: make(c - 2).wait_send())
        make(c).start()

    def start_sized(c, s, make):
        sized(s, lambda rows: start(c, lambda k: make(k, s, rows)))

    def got_gather(c, s):
        sized(s, lambda rows: down(c, s, rows).wait_recv())

    def got_back(c, slot, rows):
        ref = buf.at[1, c, slot, rows]
        remote(ref, ref, back_send.at[0, 0], rz_recv.at[c, slot], up_z, y).wait_recv()

    def valid(c):
        return (c >= 0) & (c < chunks)

    def gather_own(i):
        pl.when(valid(i))(lambda: start(i, lambda k: cross(k, z)))

        c = i - 1

        @pl.when(valid(c))
        def _():
            cross(c, z).wait_recv()
            pl.when(goes_down(z))(lambda: start_sized(c, z, down))
            pl.when(goes_up(z))(lambda: start_sized(c, z, up))

    def gather_hop(i, h):
        c = i - 1 - h
        s = z + h

        @pl.when(valid(c) & (s < planes) & (z >= low(s)))
        def _():
            got_gather(c, s)
            pl.when(goes_down(s))(lambda: start_sized(c, s, down))
            pl.when(single(s))(lambda: start(c, lambda k: cross(k, s)))

        t = lax.rem(z - h + planes, planes)

        @pl.when(valid(c) & (((z > t) & (low(t) > 0)) | ((z < t) & (z < low(t)))))
        def _():
            got_gather(c, t)
            pl.when(goes_up(t))(lambda: start_sized(c, t, up))
            pl.when((z < t) & single(t))(lambda: start(c, lambda k: cross(k, t)))

    def compute(i):
        c = i - 2 - HOPS

        @pl.when(valid(c))
        def _():
            def arrived(s):
                pl.when(single(s))(lambda: cross(c, s).wait_recv())

            loop(z + 1, planes, arrived)

            def gathered(s, total):
                return total + jnp.dot(qr[s], gt[c, s], preferred_element_type=F32)

            total = lax.fori_loop(z, planes, gathered, jnp.zeros((nb, LANES), F32))
            first[c] = total.astype(BF16)

            def share(s):
                buf[0, c, s] = jnp.dot(qrt[s], first[c], preferred_element_type=F32).astype(BF16)
                pl.when((s > z) & single(s))(lambda: start(c, lambda k: rcross(k, s)))

            loop(z, planes, share)

    def back_hop(i, h):
        c = i - 3 - HOPS - (HOPS - h)

        def contribute(s, child):
            @pl.when(single(s))
            def _():
                rcross(c, s).wait_recv()
                pl.when(child)(lambda: got_back(c, s, own))
                pl.when(child)(lambda: add(s, True))
                pl.when(jnp.logical_not(child))(lambda: add(s, False))

            @pl.when(jnp.logical_not(single(s)) & child)
            def _():
                got_back(c, s, pl.ds(0, 2 * nb))
                buf[0, c, s] = (buf[0, c, s].astype(F32) + buf[1, c, s].astype(F32)).astype(BF16)

            start_sized(c, s, back)

        def add(s, child):
            value = buf[0, c, s, own, :].astype(F32) + yin[c, s].astype(F32)
            if child:
                value = value + buf[1, c, s, own, :].astype(F32)
            buf[0, c, s, own, :] = value.astype(BF16)

        s = z + h

        @pl.when(valid(c) & (s < planes) & (z >= low(s)))
        def _():
            contribute(s, z - 1 >= low(s))

        t = lax.rem(z - h + planes, planes)

        @pl.when(valid(c) & (z < t) & (z < low(t)))
        def _():
            contribute(t, z + 1 < low(t))

        @pl.when(valid(c) & (z > t) & (low(t) > 0))
        def _():
            sized(t, lambda rows: got_back(c, t, rows))
            start_sized(c, t, back)

    def root(i):
        c = i - 3 - 2 * HOPS

        @pl.when(valid(c))
        def _():
            pl.when(z > 0)(lambda: sized(z, lambda rows: got_back(c, z, rows)))
            pl.when(low(z) > 0)(lambda: sized(z, lambda rows: got_back(c, planes, rows)))

            @pl.when((z > 0) & jnp.logical_not(single(z)))
            def _():
                buf[0, c, z, other, :] = (
                    buf[0, c, z, other, :].astype(F32) + buf[1, c, z, other, :].astype(F32)
                ).astype(BF16)

                @pl.when(low(z) > 0)
                def _():
                    buf[0, c, z, other, :] = (
                        buf[0, c, z, other, :].astype(F32) + buf[1, c, planes, other, :].astype(F32)
                    ).astype(BF16)

            start(c, lambda k: rcross(k, z))

        d = c - 1

        @pl.when(valid(d))
        def _():
            rcross(d, z).wait_recv()
            total = jnp.dot(qrt[z, own, :], first[d], preferred_element_type=F32) + yin[d, z].astype(F32)
            precond[:, :LANES] = total
            pl.when(z > 0)(lambda: gain(d, z))
            pl.when(low(z) > 0)(lambda: gain(d, planes))
            second[d] = precond[:, :LANES].astype(BF16)

    def gain(d, slot):
        precond[:, :LANES] += buf[1, d, slot, own, :].astype(F32)

    def turn(s):
        load(s).wait()
        qrt[s] = qr[s].T

    def step(i):
        gather_own(i)
        loop(1, HOPS + 1, lambda h: gather_hop(i, h))
        pl.when((2 * i < planes) & (2 * i >= z))(lambda: turn(2 * i))
        pl.when((2 * i + 1 < planes) & (2 * i + 1 >= z))(lambda: turn(2 * i + 1))
        compute(i)
        loop(1, HOPS + 1, lambda h: back_hop(i, h))
        root(i)

    loop(0, chunks + 4 + 2 * HOPS, step)

    load_ql.wait()
    sub = jnp.concatenate([second[c] for c in range(chunks)], axis=1)
    third = lax.dot_general(sub, ql[...], (((1,), (1,)), ((), ())), preferred_element_type=F32).astype(BF16)
    precond[...] = jnp.dot(third, ql[...], preferred_element_type=F32)

    value = precond[...]
    square = value * value
    tile = square[0:8]
    for r in range(8, nb, 8):
        tile = tile + square[r : r + 8]
    total = tile[:, 0:128]
    for k in range(128, value.shape[1], 128):
        total = total + tile[:, k : k + 128]
    mine[...] = total

    def exchange(phase, n, me, ident, slots):
        slots[me] = mine[...]

        def make(peer, at):
            return pltpu.make_async_remote_copy(
                src_ref=mine,
                dst_ref=slots.at[at],
                send_sem=ar_send.at[phase, peer],
                recv_sem=ar_recv.at[phase, at],
                device_id=ident(peer),
                device_id_type=MESH,
            )

        loop(1, n, lambda k: make(lax.rem(me + k, n), me).start())

        def wait(k):
            peer = lax.rem(me + k, n)
            make(peer, peer).wait_recv()

        loop(1, n, wait)
        loop(1, n, lambda k: make(lax.rem(me + k, n), me).wait_send())
        total = slots[0]
        for k in range(1, n):
            total = total + slots[k]
        mine[...] = total

    exchange(0, n_shard, shard_me, shard_id, all_shard)
    exchange(1, n_grp, grp_me, grp_id, all_grp)

    rms = jnp.sqrt(jnp.sum(mine[...], keepdims=True) / count + 1e-06)
    factor = jnp.minimum(jnp.float32(1.0), 1.1 / rms)
    out_ref[...] = (precond[...] * factor).astype(BF16)

    def drain(s):
        for c in range(chunks - 2, chunks):
            pl.when(goes_down(s))(lambda: sized(s, lambda rows: down(c, s, rows).wait_send()))
            pl.when(goes_up(s))(lambda: sized(s, lambda rows: up(c, s, rows).wait_send()))
            pl.when(crosses(s))(lambda: cross(c, s).wait_send())
            pl.when(goes_back(s))(lambda: sized(s, lambda rows: back(c, s, rows).wait_send()))
            pl.when(crosses(s))(lambda: rcross(c, s).wait_send())

    loop(0, planes, drain)


def body(sizes, gradients, left_factor, right_factor):
    rows, nb = gradients.shape[1:]
    chunks = rows // LANES
    planes = PLANES
    n_shard, n_grp = 2 * planes, sizes[0] * sizes[1] * sizes[2]
    count = gradients.shape[0] * n_grp * rows * nb * n_shard
    dma = pltpu.SemaphoreType.DMA
    turned = pl.pallas_call(
        functools.partial(kernel, count, sizes),
        out_shape=jax.ShapeDtypeStruct((nb, rows), BF16),
        in_specs=[
            pl.BlockSpec(memory_space=pltpu.VMEM),
            pl.BlockSpec(memory_space=pl.ANY),
            pl.BlockSpec(memory_space=pl.ANY),
        ],
        out_specs=pl.BlockSpec(memory_space=pltpu.VMEM),
        scratch_shapes=[
            pltpu.VMEM((chunks, planes, 2 * nb, LANES), BF16),
            pltpu.VMEM((2, chunks, planes + 1, 2 * nb, LANES), BF16),
            pltpu.VMEM((chunks, planes, nb, LANES), BF16),
            pltpu.VMEM((planes, nb, 2 * nb), BF16),
            pltpu.VMEM((planes, 2 * nb, nb), BF16),
            pltpu.VMEM((rows, rows), BF16),
            pltpu.VMEM((chunks, nb, LANES), BF16),
            pltpu.VMEM((chunks, nb, LANES), BF16),
            pltpu.VMEM((nb, rows), F32),
            pltpu.VMEM((8, 128), F32),
            pltpu.VMEM((n_shard, 8, 128), F32),
            pltpu.VMEM((n_grp, 8, 128), F32),
            dma((2, planes)),
            dma((2, planes)),
            dma((2, planes)),
            dma((2, planes)),
            dma((2, planes)),
            dma((chunks, planes)),
            dma((chunks, planes)),
            dma((chunks, planes + 1)),
            dma((chunks, planes)),
            dma((planes + 1,)),
            dma((2, max(n_shard, n_grp))),
            dma((2, max(n_shard, n_grp))),
        ],
        compiler_params=pltpu.CompilerParams(
            collective_id=0, has_side_effects=True, vmem_limit_bytes=67043328
        ),
        name="precondition",
    )(gradients[0], right_factor[0], left_factor[0])
    return turned.T[None]


def split_mesh(devices, sizes):
    return Mesh(devices.reshape(*sizes, PLANES, 2), GRP + SHARD)


def program(split, sizes):
    in_specs = (P(GRP, None, SHARD), P(GRP, None, None), P(GRP, SHARD, None))
    return jax.shard_map(
        functools.partial(body, sizes), mesh=split, in_specs=in_specs, out_specs=P(GRP, None, SHARD), check_vma=False
    )


def solution(mesh):
    sizes = (2, 4, 2)
    return program(split_mesh(mesh.devices, sizes), sizes)
```

```python
import functools

import jax
import jax.numpy as jnp
from jax import lax
from jax.experimental import pallas as pl
from jax.experimental.pallas import tpu as pltpu
from jax.sharding import Mesh
from jax.sharding import PartitionSpec as P

MESH = pl.DeviceIdType.MESH
SHARD = ("shard_0", "shard_1")
GRP = ("grp_0", "grp_1", "grp_2")
F32 = jnp.float32
BF16 = jnp.bfloat16

PLANES = 8
LANES = 128
HOPS = 4


def low(s, c, chunks):
    return jnp.where(s >= 5, s - 3, jnp.where((s == 4) & (c >= chunks // 2), 1, 0))


def loop(lower, upper, body):
    def step(i, carry):
        body(i)
        return carry

    lax.fori_loop(lower, upper, step, 0)


def kernel(
    count,
    sizes,
    g_ref,
    qr_hbm,
    ql_hbm,
    out_ref,
    gt,
    part,
    held,
    qr,
    qrt,
    ql,
    first,
    first_sum,
    share,
    second,
    leaving,
    precond,
    mine,
    all_shard,
    all_grp,
    down_send,
    up_send,
    gather_recv,
    back_send,
    back_recv,
    swap_send,
    swap_recv,
    factor_send,
    factor_recv,
    final_send,
    final_recv,
    load_sem,
    ar_send,
    ar_recv,
):
    planes, chunks = PLANES, part.shape[0]
    nb, half = g_ref.shape[0], g_ref.shape[1] // 2
    z, y = lax.axis_index("shard_0"), lax.axis_index("shard_1")
    g0, g1, g2 = lax.axis_index("grp_0"), lax.axis_index("grp_1"), lax.axis_index("grp_2")
    n1, n2 = sizes[1], sizes[2]
    n_shard, n_grp = planes * 2, sizes[0] * n1 * n2
    shard_me = z * 2 + y
    grp_me = (g0 * n1 + g1) * n2 + g2
    up_z, down_z = lax.rem(z + 1, planes), lax.rem(z + planes - 1, planes)
    own = pl.ds(pl.multiple_of(y * nb, 16), nb)
    other = pl.ds(pl.multiple_of((1 - y) * nb, 16), nb)

    def lanes(c, base=0):
        return pl.ds(pl.multiple_of(base + c * LANES, LANES), LANES)

    def shard_id(p):
        return {"shard_0": p // 2, "shard_1": lax.rem(p, 2)}

    def grp_id(p):
        return {"grp_0": p // (n1 * n2), "grp_1": lax.rem(p // n2, n1), "grp_2": lax.rem(p, n2)}

    def bottom(s, c):
        return low(s, c, chunks)

    def at_hop(h, body):
        s = z + h
        pl.when((s < planes) & (z >= bottom(s, 0)))(lambda: body(s, 0))

        @pl.when(h > 0)
        def _():
            t = lax.rem(z - h + planes, planes)
            pl.when((t > z) & (z < bottom(t, 0)))(lambda: body(t, 1))

    def load(s):
        columns = pl.ds(pl.multiple_of(s * 2 * nb, 128), 2 * nb)
        return pltpu.make_async_copy(qr_hbm.at[:, columns], qr.at[s, own], load_sem.at[s])

    load_ql = pltpu.make_async_copy(ql_hbm, ql, load_sem.at[planes])
    loop(0, HOPS + 1, lambda h: at_hop(h, lambda s, k: load(s).start()))
    load_ql.start()

    barrier = pltpu.get_barrier_semaphore()

    def greet_shard(k):
        peer = lax.rem(shard_me + k, n_shard)
        pl.semaphore_signal(barrier, inc=1, device_id=shard_id(peer), device_id_type=MESH)

    def greet_grp(k):
        peer = lax.rem(grp_me + k, n_grp)
        pl.semaphore_signal(barrier, inc=1, device_id=grp_id(peer), device_id_type=MESH)

    loop(1, n_shard, greet_shard)
    loop(1, n_grp, greet_grp)
    gt[z, own, :] = g_ref[:, pl.ds(pl.multiple_of(y * half, LANES), half)]
    pl.semaphore_wait(barrier, n_shard + n_grp - 2)

    def remote(src, dst, send, recv, to_z, to_y):
        return pltpu.make_async_remote_copy(
            src_ref=src,
            dst_ref=dst,
            send_sem=send,
            recv_sem=recv,
            device_id={"shard_0": to_z, "shard_1": to_y},
            device_id_type=MESH,
        )

    def swap(c):
        src = g_ref.at[:, lanes(c, (1 - y) * half)]
        return remote(src, gt.at[z, own, lanes(c)], swap_send.at[c], swap_recv.at[c], z, 1 - y)

    def factor(s):
        ref = qr.at[s, own]
        return remote(ref, ref, factor_send.at[s], factor_recv.at[s], z, 1 - y)

    def down(c, s):
        ref = gt.at[s, :, lanes(c)]
        return remote(ref, ref, down_send.at[c, s], gather_recv.at[c, s], down_z, y)

    def up(c, s):
        ref = gt.at[s, :, lanes(c)]
        return remote(ref, ref, up_send.at[c, s], gather_recv.at[c, s], up_z, y)

    def back(c, s, src):
        rising = (z < s) & (z >= bottom(s, c))
        parent = jnp.where(rising, up_z, down_z)
        slot = jnp.where((parent == s) & jnp.logical_not(rising), planes, s)
        return remote(src, held.at[c, slot], back_send.at[c, s], back_recv.at[c, slot], parent, y)

    def final(c):
        return remote(
            leaving.at[c], second.at[y * chunks + c], final_send.at[c], final_recv.at[c], z, 1 - y
        )

    def goes_down(c, s):
        return (z <= s) & (z - 1 >= bottom(s, c))

    def goes_up(c, s):
        return ((z >= s) & (bottom(s, c) > 0)) | ((z < s) & (z + 1 < bottom(s, c)))

    def got_back(c, slot):
        remote(held.at[c, slot], held.at[c, slot], back_send.at[0, 0], back_recv.at[c, slot], up_z, y).wait_recv()

    loop(0, chunks, lambda c: swap(c).start())

    def send_factor(s, k):
        load(s).wait()
        factor(s).start()

    loop(0, HOPS + 1, lambda h: at_hop(h, send_factor))

    def inject(c):
        @pl.when(c < chunks)
        def _():
            swap(c).wait_recv()
            pl.when(goes_down(c, z))(lambda: down(c, z).start())
            pl.when(goes_up(c, z))(lambda: up(c, z).start())

    def gather_hop(c, h):
        s = z + h

        @pl.when((c >= 0) & (c < chunks) & (s < planes) & (z >= bottom(s, c)))
        def _():
            down(c, s).wait_recv()
            pl.when(goes_down(c, s))(lambda: down(c, s).start())

        t = lax.rem(z - h + planes, planes)

        @pl.when((c >= 0) & (c < chunks) & (((z > t) & (bottom(t, c) > 0)) | ((z < t) & (z < bottom(t, c)))))
        def _():
            up(c, t).wait_recv()
            pl.when(goes_up(c, t))(lambda: up(c, t).start())

    def multiply(s, k):
        factor(s).wait_recv()
        qrt[s] = qr[s].T
        first_sum[...] += jnp.dot(qr[s], gt[s], preferred_element_type=F32)

    first_sum[...] = jnp.zeros_like(first_sum)

    def step(i):
        inject(i)
        loop(1, HOPS + 1, lambda h: gather_hop(i - h, h))
        pl.when(i >= chunks - 1)(lambda: at_hop(i - chunks + 1, multiply))

    loop(0, chunks + HOPS, step)
    first[...] = first_sum[...].astype(BF16)

    def product(s, k):
        share[k] = jnp.dot(qrt[s], first[...], preferred_element_type=F32)

    def contribute(c, s, k):
        floor = bottom(s, c)
        child = ((z >= floor) & (z - 1 >= floor)) | (z + 1 < floor)

        @pl.when(child)
        def _():
            got_back(c, s)
            part[c, s] = (share[k, :, lanes(c)] + held[c, s].astype(F32)).astype(BF16)

        @pl.when(jnp.logical_not(child))
        def _():
            part[c, s] = share[k, :, lanes(c)].astype(BF16)

        back(c, s, part.at[c, s]).start()

    def back_phase(i):
        h = HOPS - i
        at_hop(h, product)

        def send(c):
            at_hop(h, lambda s, k: contribute(c, s, k))
            t = z - h

            @pl.when((t >= 0) & (bottom(t, c) > 0))
            def _():
                got_back(c, t)
                back(c, t, held.at[c, t]).start()

        loop(0, chunks, send)

    loop(0, HOPS, back_phase)

    product(z, 0)

    def finish(c):
        @pl.when(z > 0)
        def _():
            got_back(c, z)
            share[0, :, lanes(c)] += held[c, z].astype(F32)

        @pl.when(bottom(z, c) > 0)
        def _():
            got_back(c, planes)
            share[0, :, lanes(c)] += held[c, planes].astype(F32)

        leaving[c] = share[0, other, lanes(c)].astype(BF16)
        final(c).start()
        second[y * chunks + c] = share[0, own, lanes(c)].astype(BF16)

    loop(0, chunks, finish)

    load_ql.wait()
    loop(0, chunks, lambda c: final(c).wait_recv())
    sub = jnp.concatenate([second[c] for c in range(2 * chunks)], axis=1)
    third = lax.dot_general(sub, ql[...], (((1,), (1,)), ((), ())), preferred_element_type=F32).astype(BF16)
    precond[...] = jnp.dot(third, ql[...], preferred_element_type=F32)

    value = precond[...]
    square = value * value
    tile = square[0:8]
    for r in range(8, nb, 8):
        tile = tile + square[r : r + 8]
    total = tile[:, 0:128]
    for k in range(128, value.shape[1], 128):
        total = total + tile[:, k : k + 128]
    mine[...] = total

    def exchange(phase, n, me, ident, slots):
        slots[me] = mine[...]

        def make(peer, at):
            return pltpu.make_async_remote_copy(
                src_ref=mine,
                dst_ref=slots.at[at],
                send_sem=ar_send.at[phase, peer],
                recv_sem=ar_recv.at[phase, at],
                device_id=ident(peer),
                device_id_type=MESH,
            )

        loop(1, n, lambda k: make(lax.rem(me + k, n), me).start())

        def wait(k):
            peer = lax.rem(me + k, n)
            make(peer, peer).wait_recv()

        loop(1, n, wait)
        loop(1, n, lambda k: make(lax.rem(me + k, n), me).wait_send())
        total = slots[0]
        for k in range(1, n):
            total = total + slots[k]
        mine[...] = total

    exchange(0, n_shard, shard_me, shard_id, all_shard)
    exchange(1, n_grp, grp_me, grp_id, all_grp)

    rms = jnp.sqrt(jnp.sum(mine[...], keepdims=True) / count + 1e-06)
    scale = jnp.minimum(jnp.float32(1.0), 1.1 / rms)
    out_ref[...] = (precond[...] * scale).astype(BF16)

    def drain(c):
        swap(c).wait_send()
        final(c).wait_send()

        def each(s):
            pl.when(goes_down(c, s))(lambda: down(c, s).wait_send())
            pl.when(goes_up(c, s))(lambda: up(c, s).wait_send())
            pl.when((z < s) | ((z > s) & (bottom(s, c) > 0)))(lambda: back(c, s, part.at[c, s]).wait_send())

        loop(0, planes, each)

    loop(0, chunks, drain)
    loop(z, planes, lambda s: factor(s).wait_send())


def body(sizes, gradients, left_factor, right_factor):
    rows, nb = gradients.shape[1:]
    half = rows // 2
    chunks = half // LANES
    planes = PLANES
    n_shard, n_grp = 2 * planes, sizes[0] * sizes[1] * sizes[2]
    count = gradients.shape[0] * n_grp * rows * nb * n_shard
    dma = pltpu.SemaphoreType.DMA
    turned = pl.pallas_call(
        functools.partial(kernel, count, sizes),
        out_shape=jax.ShapeDtypeStruct((nb, rows), BF16),
        in_specs=[
            pl.BlockSpec(memory_space=pltpu.VMEM),
            pl.BlockSpec(memory_space=pl.ANY),
            pl.BlockSpec(memory_space=pl.ANY),
        ],
        out_specs=pl.BlockSpec(memory_space=pltpu.VMEM),
        scratch_shapes=[
            pltpu.VMEM((planes, 2 * nb, half), BF16),
            pltpu.VMEM((chunks, planes, 2 * nb, LANES), BF16),
            pltpu.VMEM((chunks, planes + 1, 2 * nb, LANES), BF16),
            pltpu.VMEM((planes, 2 * nb, 2 * nb), BF16),
            pltpu.VMEM((planes, 2 * nb, 2 * nb), BF16),
            pltpu.VMEM((rows, rows), BF16),
            pltpu.VMEM((2 * nb, half), BF16),
            pltpu.VMEM((2 * nb, half), F32),
            pltpu.VMEM((2, 2 * nb, half), F32),
            pltpu.VMEM((2 * chunks, nb, LANES), BF16),
            pltpu.VMEM((chunks, nb, LANES), BF16),
            pltpu.VMEM((nb, rows), F32),
            pltpu.VMEM((8, 128), F32),
            pltpu.VMEM((n_shard, 8, 128), F32),
            pltpu.VMEM((n_grp, 8, 128), F32),
            dma((chunks, planes)),
            dma((chunks, planes)),
            dma((chunks, planes)),
            dma((chunks, planes)),
            dma((chunks, planes + 1)),
            dma((chunks,)),
            dma((chunks,)),
            dma((planes,)),
            dma((planes,)),
            dma((chunks,)),
            dma((chunks,)),
            dma((planes + 1,)),
            dma((2, max(n_shard, n_grp))),
            dma((2, max(n_shard, n_grp))),
        ],
        compiler_params=pltpu.CompilerParams(
            collective_id=0, has_side_effects=True, vmem_limit_bytes=67043328
        ),
        name="precondition",
    )(gradients[0].T, right_factor[0], left_factor[0])
    return turned.T[None]


def split_mesh(devices, sizes):
    return Mesh(devices.reshape(*sizes, PLANES, 2), GRP + SHARD)


def program(split, sizes):
    in_specs = (P(GRP, None, SHARD), P(GRP, None, None), P(GRP, SHARD, None))
    return jax.shard_map(
        functools.partial(body, sizes), mesh=split, in_specs=in_specs, out_specs=P(GRP, None, SHARD), check_vma=False
    )


def solution(mesh):
    sizes = (2, 4, 2)
    return program(split_mesh(mesh.devices, sizes), sizes)
```

```python
import functools

import jax
import jax.numpy as jnp
from jax import lax
from jax.experimental import pallas as pl
from jax.experimental.pallas import tpu as pltpu
from jax.sharding import Mesh
from jax.sharding import PartitionSpec as P

MESH = pl.DeviceIdType.MESH
SHARD = ("shard_0", "shard_1")
GRP = ("grp_0", "grp_1", "grp_2")
F32 = jnp.float32
BF16 = jnp.bfloat16

PLANES = 8
LANES = 128
HOPS = 4


def low(s, c, chunks):
    return jnp.where(s >= 5, s - 3, jnp.where((s == 4) & (c >= chunks // 2), 1, 0))


def loop(lower, upper, body):
    def step(i, carry):
        body(i)
        return carry

    lax.fori_loop(lower, upper, step, 0)


def kernel(
    count,
    sizes,
    g_ref,
    qr_hbm,
    ql_hbm,
    out_ref,
    gt,
    part,
    held,
    qr,
    qrt,
    ql,
    first,
    first_sum,
    share,
    second,
    leaving,
    relay_in,
    relay_out,
    precond,
    mine,
    all_shard,
    all_grp,
    down_send,
    up_send,
    gather_recv,
    piece_send,
    piece_recv,
    back_send,
    back_recv,
    swap_send,
    swap_recv,
    factor_send,
    factor_recv,
    relay_send,
    relay_recv,
    final_send,
    final_recv,
    load_sem,
    ar_send,
    ar_recv,
):
    planes, chunks = PLANES, part.shape[0]
    nb, half = g_ref.shape[0], g_ref.shape[1] // 2
    z, y = lax.axis_index("shard_0"), lax.axis_index("shard_1")
    g0, g1, g2 = lax.axis_index("grp_0"), lax.axis_index("grp_1"), lax.axis_index("grp_2")
    n1, n2 = sizes[1], sizes[2]
    n_shard, n_grp = planes * 2, sizes[0] * n1 * n2
    shard_me = z * 2 + y
    grp_me = (g0 * n1 + g1) * n2 + g2
    up_z, down_z = lax.rem(z + 1, planes), lax.rem(z + planes - 1, planes)
    own = pl.ds(pl.multiple_of(y * nb, 16), nb)
    other = pl.ds(pl.multiple_of((1 - y) * nb, 16), nb)

    def lanes(c, base=0):
        return pl.ds(pl.multiple_of(base + c * LANES, LANES), LANES)

    def shard_id(p):
        return {"shard_0": p // 2, "shard_1": lax.rem(p, 2)}

    def grp_id(p):
        return {"grp_0": p // (n1 * n2), "grp_1": lax.rem(p // n2, n1), "grp_2": lax.rem(p, n2)}

    def bottom(s, c):
        return low(s, c, chunks)

    def at_hop(h, body):
        s = z + h
        pl.when((s < planes) & (z >= bottom(s, 0)))(lambda: body(s, 0))

        @pl.when(h > 0)
        def _():
            t = lax.rem(z - h + planes, planes)
            pl.when((t > z) & (z < bottom(t, 0)))(lambda: body(t, 1))

    def load(s):
        columns = pl.ds(pl.multiple_of(s * 2 * nb, 128), 2 * nb)
        return pltpu.make_async_copy(qr_hbm.at[:, columns], qr.at[s, own], load_sem.at[s])

    load_ql = pltpu.make_async_copy(ql_hbm, ql, load_sem.at[planes])
    loop(0, HOPS + 1, lambda h: at_hop(h, lambda s, k: load(s).start()))
    load_ql.start()

    barrier = pltpu.get_barrier_semaphore()

    def greet_shard(k):
        peer = lax.rem(shard_me + k, n_shard)
        pl.semaphore_signal(barrier, inc=1, device_id=shard_id(peer), device_id_type=MESH)

    def greet_grp(k):
        peer = lax.rem(grp_me + k, n_grp)
        pl.semaphore_signal(barrier, inc=1, device_id=grp_id(peer), device_id_type=MESH)

    loop(1, n_shard, greet_shard)
    loop(1, n_grp, greet_grp)
    gt[z, own, :] = g_ref[:, pl.ds(pl.multiple_of(y * half, LANES), half)]
    pl.semaphore_wait(barrier, n_shard + n_grp - 2)

    def remote(src, dst, send, recv, to_z, to_y):
        return pltpu.make_async_remote_copy(
            src_ref=src,
            dst_ref=dst,
            send_sem=send,
            recv_sem=recv,
            device_id={"shard_0": to_z, "shard_1": to_y},
            device_id_type=MESH,
        )

    def swap(c):
        src = g_ref.at[:, lanes(c, (1 - y) * half)]
        return remote(src, gt.at[z, own, lanes(c)], swap_send.at[c], swap_recv.at[c], z, 1 - y)

    def factor(s):
        ref = qr.at[s, own]
        return remote(ref, ref, factor_send.at[s], factor_recv.at[s], z, 1 - y)

    def down(c, s):
        ref = gt.at[s, :, lanes(c)]
        return remote(ref, ref, down_send.at[c, s], gather_recv.at[c, s], down_z, y)

    def up(c, s):
        ref = gt.at[s, :, lanes(c)]
        return remote(ref, ref, up_send.at[c, s], gather_recv.at[c, s], up_z, y)

    def back(c, s, src):
        rising = (z < s) & (z >= bottom(s, c))
        parent = jnp.where(rising, up_z, down_z)
        slot = jnp.where((parent == s) & jnp.logical_not(rising), planes, s)
        return remote(src, held.at[c, slot], back_send.at[c, s], back_recv.at[c, slot], parent, y)

    def final(c):
        return remote(
            leaving.at[c], second.at[y * chunks + c], final_send.at[c], final_recv.at[c], z, 1 - y
        )

    def goes_down(s):
        return (z <= s) & (z - 1 >= bottom(s, 0))

    def goes_up(s):
        return ((z >= s) & (bottom(s, 0) > 0)) | ((z < s) & (z + 1 < bottom(s, 0)))

    def got_back(c, slot):
        remote(held.at[c, slot], held.at[c, slot], back_send.at[0, 0], back_recv.at[c, slot], up_z, y).wait_recv()

    def relayed(s):
        return ((z <= 2) & (s == z + 4)) | ((z == 0) & (s == 5))

    def relays(k):
        return (z == 7) | ((k == 0) & ((z == 2) | (z == 3)))

    def relay_slot(s):
        return jnp.where((z == 0) & (s == 4), 1, 0)

    def relay_first(s, k):
        via = jnp.where(z == 0, down_z, up_z)
        return remote(qr.at[s, own], relay_in.at[k], relay_send.at[0, k], relay_recv.at[0, k], via, y)

    def relay_second(k):
        return remote(relay_in.at[k], relay_out.at[k], relay_send.at[1, k], relay_recv.at[1, k], z, 1 - y)

    def relay_third(k):
        s = jnp.where(z == 7, 5 - k, z + 3)
        to = jnp.where(z == 7, up_z, down_z)
        return remote(relay_out.at[k], qr.at[s, other], relay_send.at[2, k], factor_recv.at[s], to, y)

    def start_relay(s, k):
        @pl.when(relayed(s))
        def _():
            load(s).wait()
            relay_first(s, relay_slot(s)).start()

    def send_factor(s, k):
        @pl.when(jnp.logical_not(relayed(s)))
        def _():
            load(s).wait()
            factor(s).start()

    def relay_on(k):
        @pl.when(relays(k))
        def _():
            relay_first(z, k).wait_recv()
            relay_second(k).start()

    def relay_home(k):
        @pl.when(relays(k))
        def _():
            relay_second(k).wait_recv()
            relay_third(k).start()

    def piece(c, way, k, s):
        ref = gt.at[s, own if k == 0 else other, lanes(c)]
        return remote(ref, ref, piece_send.at[way, k, c], piece_recv.at[way, k, c], (down_z, up_z)[way], y)

    def start_pieces(c, k):
        pl.when(goes_down(z))(lambda: piece(c, 0, k, z).start())
        pl.when(goes_up(z))(lambda: piece(c, 1, k, z).start())

    def inject(c):
        swap(c).wait_recv()
        start_pieces(c, 1)

    def gather_hop(h, arrive):
        def chunk(c):
            s = z + h

            @pl.when((s < planes) & (z >= bottom(s, 0)))
            def _():
                arrive(c, 0, s)
                pl.when(goes_down(s))(lambda: down(c, s).start())

            t = lax.rem(z - h + planes, planes)

            @pl.when(((z > t) & (bottom(t, 0) > 0)) | ((z < t) & (z < bottom(t, 0))))
            def _():
                arrive(c, 1, t)
                pl.when(goes_up(t))(lambda: up(c, t).start())

        loop(0, chunks, chunk)

    def arrive_pieces(c, way, s):
        piece(c, way, 0, s).wait_recv()
        piece(c, way, 1, s).wait_recv()

    def arrive_whole(c, way, s):
        down(c, s).wait_recv()

    def multiply(s, k):
        factor(s).wait_recv()
        first_sum[...] += jnp.dot(qr[s], gt[s], preferred_element_type=F32)

    loop(0, chunks, lambda c: swap(c).start())
    at_hop(0, send_factor)
    loop(HOPS - 1, HOPS + 1, lambda h: at_hop(h, start_relay))
    loop(0, chunks, lambda c: start_pieces(c, 0))
    loop(0, chunks, inject)
    relay_on(0)
    loop(1, HOPS + 1, lambda h: at_hop(h, send_factor))
    first_sum[...] = jnp.zeros_like(first_sum)
    gather_hop(1, arrive_pieces)
    relay_on(1)
    relay_home(0)
    at_hop(0, multiply)

    def hop(h):
        gather_hop(h, arrive_whole)
        pl.when(h == 2)(lambda: relay_home(1))
        at_hop(h - 1, multiply)

    loop(2, HOPS + 1, hop)
    at_hop(HOPS, multiply)
    first[...] = first_sum[...].astype(BF16)

    def product(s, k):
        qrt[s] = qr[s].T
        share[k] = jnp.dot(qrt[s], first[...], preferred_element_type=F32)

    def contribute(c, s, k):
        floor = bottom(s, c)
        child = ((z >= floor) & (z - 1 >= floor)) | (z + 1 < floor)

        @pl.when(child)
        def _():
            got_back(c, s)
            part[c, s] = (share[k, :, lanes(c)] + held[c, s].astype(F32)).astype(BF16)

        @pl.when(jnp.logical_not(child))
        def _():
            part[c, s] = share[k, :, lanes(c)].astype(BF16)

        back(c, s, part.at[c, s]).start()

    def back_phase(i):
        h = HOPS - i
        at_hop(h, product)

        def send(c):
            at_hop(h, lambda s, k: contribute(c, s, k))
            t = z - h

            @pl.when((t >= 0) & (bottom(t, c) > 0))
            def _():
                got_back(c, t)
                back(c, t, held.at[c, t]).start()

        loop(0, chunks, send)

    loop(0, HOPS, back_phase)

    product(z, 0)

    def finish(c):
        @pl.when(z > 0)
        def _():
            got_back(c, z)
            share[0, :, lanes(c)] += held[c, z].astype(F32)

        @pl.when(bottom(z, c) > 0)
        def _():
            got_back(c, planes)
            share[0, :, lanes(c)] += held[c, planes].astype(F32)

        leaving[c] = share[0, other, lanes(c)].astype(BF16)
        final(c).start()
        second[y * chunks + c] = share[0, own, lanes(c)].astype(BF16)

    loop(0, chunks, finish)

    load_ql.wait()
    loop(0, chunks, lambda c: final(c).wait_recv())
    sub = jnp.concatenate([second[c] for c in range(2 * chunks)], axis=1)
    third = lax.dot_general(sub, ql[...], (((1,), (1,)), ((), ())), preferred_element_type=F32).astype(BF16)
    precond[...] = jnp.dot(third, ql[...], preferred_element_type=F32)

    value = precond[...]
    square = value * value
    tile = square[0:8]
    for r in range(8, nb, 8):
        tile = tile + square[r : r + 8]
    total = tile[:, 0:128]
    for k in range(128, value.shape[1], 128):
        total = total + tile[:, k : k + 128]
    mine[...] = total

    def exchange(phase, n, me, ident, slots):
        slots[me] = mine[...]

        def make(peer, at):
            return pltpu.make_async_remote_copy(
                src_ref=mine,
                dst_ref=slots.at[at],
                send_sem=ar_send.at[phase, peer],
                recv_sem=ar_recv.at[phase, at],
                device_id=ident(peer),
                device_id_type=MESH,
            )

        loop(1, n, lambda k: make(lax.rem(me + k, n), me).start())

        def wait(k):
            peer = lax.rem(me + k, n)
            make(peer, peer).wait_recv()

        loop(1, n, wait)
        loop(1, n, lambda k: make(lax.rem(me + k, n), me).wait_send())
        total = slots[0]
        for k in range(1, n):
            total = total + slots[k]
        mine[...] = total

    exchange(0, n_shard, shard_me, shard_id, all_shard)
    exchange(1, n_grp, grp_me, grp_id, all_grp)

    rms = jnp.sqrt(jnp.sum(mine[...], keepdims=True) / count + 1e-06)
    scale = jnp.minimum(jnp.float32(1.0), 1.1 / rms)
    out_ref[...] = (precond[...] * scale).astype(BF16)

    def drain(c):
        swap(c).wait_send()
        final(c).wait_send()
        for k in range(2):
            pl.when(goes_down(z))(lambda: piece(c, 0, k, z).wait_send())
            pl.when(goes_up(z))(lambda: piece(c, 1, k, z).wait_send())

        def each(s):
            pl.when(goes_down(s) & (s != z))(lambda: down(c, s).wait_send())
            pl.when(goes_up(s) & (s != z))(lambda: up(c, s).wait_send())
            pl.when((z < s) | ((z > s) & (bottom(s, c) > 0)))(lambda: back(c, s, part.at[c, s]).wait_send())

        loop(0, planes, each)

    loop(0, chunks, drain)

    def drain_factor(s):
        pl.when(relayed(s))(lambda: relay_first(s, relay_slot(s)).wait_send())
        pl.when(jnp.logical_not(relayed(s)))(lambda: factor(s).wait_send())

    def drain_relay(k):
        @pl.when(relays(k))
        def _():
            relay_second(k).wait_send()
            relay_third(k).wait_send()

    loop(z, planes, drain_factor)
    loop(0, 2, drain_relay)


def body(sizes, gradients, left_factor, right_factor):
    rows, nb = gradients.shape[1:]
    half = rows // 2
    chunks = half // LANES
    planes = PLANES
    n_shard, n_grp = 2 * planes, sizes[0] * sizes[1] * sizes[2]
    count = gradients.shape[0] * n_grp * rows * nb * n_shard
    dma = pltpu.SemaphoreType.DMA
    turned = pl.pallas_call(
        functools.partial(kernel, count, sizes),
        out_shape=jax.ShapeDtypeStruct((nb, rows), BF16),
        in_specs=[
            pl.BlockSpec(memory_space=pltpu.VMEM),
            pl.BlockSpec(memory_space=pl.ANY),
            pl.BlockSpec(memory_space=pl.ANY),
        ],
        out_specs=pl.BlockSpec(memory_space=pltpu.VMEM),
        scratch_shapes=[
            pltpu.VMEM((planes, 2 * nb, half), BF16),
            pltpu.VMEM((chunks, planes, 2 * nb, LANES), BF16),
            pltpu.VMEM((chunks, planes + 1, 2 * nb, LANES), BF16),
            pltpu.VMEM((planes, 2 * nb, 2 * nb), BF16),
            pltpu.VMEM((planes, 2 * nb, 2 * nb), BF16),
            pltpu.VMEM((rows, rows), BF16),
            pltpu.VMEM((2 * nb, half), BF16),
            pltpu.VMEM((2 * nb, half), F32),
            pltpu.VMEM((2, 2 * nb, half), F32),
            pltpu.VMEM((2 * chunks, nb, LANES), BF16),
            pltpu.VMEM((chunks, nb, LANES), BF16),
            pltpu.VMEM((2, nb, 2 * nb), BF16),
            pltpu.VMEM((2, nb, 2 * nb), BF16),
            pltpu.VMEM((nb, rows), F32),
            pltpu.VMEM((8, 128), F32),
            pltpu.VMEM((n_shard, 8, 128), F32),
            pltpu.VMEM((n_grp, 8, 128), F32),
            dma((chunks, planes)),
            dma((chunks, planes)),
            dma((chunks, planes)),
            dma((2, 2, chunks)),
            dma((2, 2, chunks)),
            dma((chunks, planes)),
            dma((chunks, planes + 1)),
            dma((chunks,)),
            dma((chunks,)),
            dma((planes,)),
            dma((planes,)),
            dma((3, 2)),
            dma((2, 2)),
            dma((chunks,)),
            dma((chunks,)),
            dma((planes + 1,)),
            dma((2, max(n_shard, n_grp))),
            dma((2, max(n_shard, n_grp))),
        ],
        compiler_params=pltpu.CompilerParams(
            collective_id=0, has_side_effects=True, vmem_limit_bytes=67043328
        ),
        name="precondition",
    )(gradients[0].T, right_factor[0], left_factor[0])
    return turned.T[None]


def split_mesh(devices, sizes):
    return Mesh(devices.reshape(*sizes, PLANES, 2), GRP + SHARD)


def program(split, sizes):
    in_specs = (P(GRP, None, SHARD), P(GRP, None, None), P(GRP, SHARD, None))
    return jax.shard_map(
        functools.partial(body, sizes), mesh=split, in_specs=in_specs, out_specs=P(GRP, None, SHARD), check_vma=False
    )


def solution(mesh):
    sizes = (2, 4, 2)
    return program(split_mesh(mesh.devices, sizes), sizes)
```

```python
import functools

import jax
import jax.numpy as jnp
from jax import lax
from jax.experimental import pallas as pl
from jax.experimental.pallas import tpu as pltpu
from jax.sharding import Mesh
from jax.sharding import PartitionSpec as P

MESH = pl.DeviceIdType.MESH
SHARD = ("shard_0", "shard_1")
GRP = ("grp_0", "grp_1", "grp_2")
F32 = jnp.float32
BF16 = jnp.bfloat16

PLANES = 8
LANES = 128
HOPS = 4


def low(s, c, chunks):
    return jnp.where(s >= 5, s - 3, jnp.where((s == 4) & (c >= chunks // 2), 1, 0))


def loop(lower, upper, body):
    def step(i, carry):
        body(i)
        return carry

    lax.fori_loop(lower, upper, step, 0)


def kernel(
    count,
    sizes,
    g_ref,
    qr_hbm,
    ql_hbm,
    out_ref,
    gt,
    part,
    held,
    qr,
    qrt,
    ql,
    first,
    first_sum,
    share,
    second,
    leaving,
    coming,
    kept,
    landed,
    swapped,
    relay_in,
    relay_out,
    precond,
    mine,
    all_shard,
    all_grp,
    down_send,
    up_send,
    gather_recv,
    piece_send,
    piece_recv,
    back_send,
    back_recv,
    last_send,
    landed_recv,
    swap_send,
    swap_recv,
    factor_send,
    factor_recv,
    relay_send,
    relay_recv,
    final_send,
    final_recv,
    load_sem,
    ar_send,
    ar_recv,
):
    planes, chunks = PLANES, part.shape[0]
    nb, half = leaving.shape[1], first.shape[1]
    z, y = lax.axis_index("shard_0"), lax.axis_index("shard_1")
    g0, g1, g2 = lax.axis_index("grp_0"), lax.axis_index("grp_1"), lax.axis_index("grp_2")
    n1, n2 = sizes[1], sizes[2]
    n_shard, n_grp = planes * 2, sizes[0] * n1 * n2
    shard_me = z * 2 + y
    grp_me = (g0 * n1 + g1) * n2 + g2
    up_z, down_z = lax.rem(z + 1, planes), lax.rem(z + planes - 1, planes)
    own = pl.ds(pl.multiple_of(y * nb, 16), nb)
    other = pl.ds(pl.multiple_of((1 - y) * nb, 16), nb)

    def lanes(c, base=0):
        return pl.ds(pl.multiple_of(base + c * LANES, LANES), LANES)

    def shard_id(p):
        return {"shard_0": p // 2, "shard_1": lax.rem(p, 2)}

    def grp_id(p):
        return {"grp_0": p // (n1 * n2), "grp_1": lax.rem(p // n2, n1), "grp_2": lax.rem(p, n2)}

    def bottom(s, c):
        return low(s, c, chunks)

    def at_hop(h, body):
        s = z + h
        pl.when((s < planes) & (z >= bottom(s, 0)))(lambda: body(s, 0))

        @pl.when(h > 0)
        def _():
            t = lax.rem(z - h + planes, planes)
            pl.when((t > z) & (z < bottom(t, 0)))(lambda: body(t, 1))

    def load(s):
        columns = pl.ds(pl.multiple_of(s * 2 * nb, 128), 2 * nb)
        return pltpu.make_async_copy(qr_hbm.at[:, columns], qr.at[s, own], load_sem.at[s])

    load_ql = pltpu.make_async_copy(ql_hbm, ql, load_sem.at[planes])
    mine_half = pl.ds(pl.multiple_of(y * half, LANES), half)
    swap_half = pl.ds(pl.multiple_of((1 - y) * half, LANES), half)
    load_mine = pltpu.make_async_copy(g_ref.at[:, mine_half], gt.at[z, own], load_sem.at[planes + 1])
    load_swap = pltpu.make_async_copy(g_ref.at[:, swap_half], swapped, load_sem.at[planes + 2])
    load_swap.start()
    load_mine.start()
    loop(0, HOPS + 1, lambda h: at_hop(h, lambda s, k: load(s).start()))
    load_ql.start()

    barrier = pltpu.get_barrier_semaphore()

    def greet_shard(k):
        peer = lax.rem(shard_me + k, n_shard)
        pl.semaphore_signal(barrier, inc=1, device_id=shard_id(peer), device_id_type=MESH)

    def greet_grp(k):
        peer = lax.rem(grp_me + k, n_grp)
        pl.semaphore_signal(barrier, inc=1, device_id=grp_id(peer), device_id_type=MESH)

    loop(1, n_shard, greet_shard)
    loop(1, n_grp, greet_grp)
    load_swap.wait()
    load_mine.wait()
    pl.semaphore_wait(barrier, n_shard + n_grp - 2)

    def remote(src, dst, send, recv, to_z, to_y):
        return pltpu.make_async_remote_copy(
            src_ref=src,
            dst_ref=dst,
            send_sem=send,
            recv_sem=recv,
            device_id={"shard_0": to_z, "shard_1": to_y},
            device_id_type=MESH,
        )

    def swap(c):
        return remote(swapped.at[:, lanes(c)], gt.at[z, own, lanes(c)], swap_send.at[c], swap_recv.at[c], z, 1 - y)

    def factor(s):
        ref = qr.at[s, own]
        return remote(ref, ref, factor_send.at[s], factor_recv.at[s], z, 1 - y)

    def down(c, s):
        ref = gt.at[s, :, lanes(c)]
        return remote(ref, ref, down_send.at[c, s], gather_recv.at[c, s], down_z, y)

    def up(c, s):
        ref = gt.at[s, :, lanes(c)]
        return remote(ref, ref, up_send.at[c, s], gather_recv.at[c, s], up_z, y)

    def back(c, s, src):
        rising = (z < s) & (z >= bottom(s, c))
        parent = jnp.where(rising, up_z, down_z)
        return remote(src, held.at[c, s], back_send.at[c, s], back_recv.at[c, s], parent, y)

    def last(c, way, k, src):
        to_z = (up_z, down_z)[way]
        send, recv = last_send.at[way, k, c], landed_recv.at[way, y, c]
        return remote(src, landed.at[way, y, c], send, recv, to_z, y if k == 0 else 1 - y)

    def start_last(c, way, ref):
        last(c, way, 0, ref.at[own]).start()
        last(c, way, 1, ref.at[other]).start()

    def final(c):
        return remote(leaving.at[c], coming.at[c], final_send.at[c], final_recv.at[c], z, 1 - y)

    def goes_down(s):
        return (z <= s) & (z - 1 >= bottom(s, 0))

    def goes_up(s):
        return ((z >= s) & (bottom(s, 0) > 0)) | ((z < s) & (z + 1 < bottom(s, 0)))

    def got_back(c, s):
        remote(held.at[c, s], held.at[c, s], back_send.at[0, 0], back_recv.at[c, s], up_z, y).wait_recv()

    def relayed(s):
        return ((z <= 2) & (s == z + 4)) | ((z == 0) & (s == 5))

    def relays(k):
        return (z == 7) | ((k == 0) & ((z == 2) | (z == 3)))

    def relay_slot(s):
        return jnp.where((z == 0) & (s == 4), 1, 0)

    def relay_first(s, k):
        via = jnp.where(z == 0, down_z, up_z)
        return remote(qr.at[s, own], relay_in.at[k], relay_send.at[0, k], relay_recv.at[0, k], via, y)

    def relay_second(k):
        return remote(relay_in.at[k], relay_out.at[k], relay_send.at[1, k], relay_recv.at[1, k], z, 1 - y)

    def relay_third(k):
        s = jnp.where(z == 7, 5 - k, z + 3)
        to = jnp.where(z == 7, up_z, down_z)
        return remote(relay_out.at[k], qr.at[s, other], relay_send.at[2, k], factor_recv.at[s], to, y)

    def start_relay(s, k):
        @pl.when(relayed(s))
        def _():
            load(s).wait()
            relay_first(s, relay_slot(s)).start()

    def send_factor(s, k):
        @pl.when(jnp.logical_not(relayed(s)))
        def _():
            load(s).wait()
            factor(s).start()

    def relay_on(k):
        @pl.when(relays(k))
        def _():
            relay_first(z, k).wait_recv()
            relay_second(k).start()

    def relay_home(k):
        @pl.when(relays(k))
        def _():
            relay_second(k).wait_recv()
            relay_third(k).start()

    def piece(c, way, k, s):
        ref = gt.at[s, own if k == 0 else other, lanes(c)]
        return remote(ref, ref, piece_send.at[way, k, c], piece_recv.at[way, k, c], (down_z, up_z)[way], y)

    def start_pieces(c, k):
        pl.when(goes_down(z))(lambda: piece(c, 0, k, z).start())
        pl.when(goes_up(z))(lambda: piece(c, 1, k, z).start())

    def inject(c):
        swap(c).wait_recv()
        start_pieces(c, 1)

    def gather_hop(h, arrive):
        def chunk(c):
            s = z + h

            @pl.when((s < planes) & (z >= bottom(s, 0)))
            def _():
                arrive(c, 0, s)
                pl.when(goes_down(s))(lambda: down(c, s).start())

            t = lax.rem(z - h + planes, planes)

            @pl.when(((z > t) & (bottom(t, 0) > 0)) | ((z < t) & (z < bottom(t, 0))))
            def _():
                arrive(c, 1, t)
                pl.when(goes_up(t))(lambda: up(c, t).start())

        loop(0, chunks, chunk)

    def arrive_pieces(c, way, s):
        piece(c, way, 0, s).wait_recv()
        piece(c, way, 1, s).wait_recv()

    def arrive_whole(c, way, s):
        down(c, s).wait_recv()

    def multiply_own(s, k):
        first_sum[own, :] += jnp.dot(qr[s, own, :], gt[s], preferred_element_type=F32)

    def multiply_other(s, k):
        factor(s).wait_recv()
        first_sum[other, :] += jnp.dot(qr[s, other, :], gt[s], preferred_element_type=F32)

    loop(0, chunks, lambda c: swap(c).start())
    at_hop(0, send_factor)
    loop(HOPS - 1, HOPS + 1, lambda h: at_hop(h, start_relay))
    loop(0, chunks, lambda c: start_pieces(c, 0))
    loop(0, chunks, inject)
    relay_on(0)
    loop(1, HOPS + 1, lambda h: at_hop(h, send_factor))
    first_sum[...] = jnp.zeros_like(first_sum)
    gather_hop(1, arrive_pieces)
    relay_on(1)
    relay_home(0)
    at_hop(0, multiply_own)
    at_hop(1, multiply_own)
    at_hop(0, multiply_other)

    def hop(h):
        gather_hop(h, arrive_whole)
        pl.when(h == 2)(lambda: relay_home(1))
        at_hop(h, multiply_own)
        at_hop(h - 1, multiply_other)

    loop(2, HOPS + 1, hop)
    at_hop(HOPS, multiply_other)
    first[...] = first_sum[...].astype(BF16)

    def product(s, k):
        qrt[s] = qr[s].T
        share[k] = jnp.dot(qrt[s], first[...], preferred_element_type=F32)

    def contribute(c, s, k, send):
        floor = bottom(s, c)
        child = ((z >= floor) & (z - 1 >= floor)) | (z + 1 < floor)

        @pl.when(child)
        def _():
            got_back(c, s)
            part[c, s] = (share[k, :, lanes(c)] + held[c, s].astype(F32)).astype(BF16)

        @pl.when(jnp.logical_not(child))
        def _():
            part[c, s] = share[k, :, lanes(c)].astype(BF16)

        send(c, s, k, part.at[c, s])

    def back_phase(h, send):
        at_hop(h, product)

        def chunk(c):
            at_hop(h, lambda s, k: contribute(c, s, k, send))
            t = z - h

            @pl.when((t >= 0) & (bottom(t, c) > 0))
            def _():
                got_back(c, t)
                send(c, t, 1, held.at[c, t])

        loop(0, chunks, chunk)

    def send_back(c, s, k, ref):
        back(c, s, ref).start()

    def send_last(c, s, k, ref):
        start_last(c, k, ref)

    loop(0, HOPS - 2, lambda i: back_phase(HOPS - i, send_back))

    product(z, 0)
    kept[...] = share[0, own, :]

    def leave(c):
        leaving[c] = share[0, other, lanes(c)]
        final(c).start()

    loop(0, chunks, leave)
    back_phase(2, send_back)
    back_phase(1, send_last)

    def arrived(way, line, c):
        return remote(
            landed.at[way, line, c],
            landed.at[way, line, c],
            last_send.at[0, 0, 0],
            landed_recv.at[way, line, c],
            up_z,
            y,
        )

    def finish(c):
        final(c).wait_recv()

        @pl.when(z > 0)
        def _():
            arrived(0, y, c).wait_recv()
            arrived(0, 1 - y, c).wait_recv()
            kept[:, lanes(c)] += landed[0, y, c].astype(F32)
            coming[c] += landed[0, 1 - y, c].astype(F32)

        @pl.when(bottom(z, c) > 0)
        def _():
            arrived(1, y, c).wait_recv()
            arrived(1, 1 - y, c).wait_recv()
            kept[:, lanes(c)] += landed[1, y, c].astype(F32)
            coming[c] += landed[1, 1 - y, c].astype(F32)

        second[y * chunks + c] = kept[:, lanes(c)].astype(BF16)
        second[(1 - y) * chunks + c] = coming[c].astype(BF16)

    loop(0, chunks, finish)

    load_ql.wait()
    sub = jnp.concatenate([second[c] for c in range(2 * chunks)], axis=1)
    third = lax.dot_general(sub, ql[...], (((1,), (1,)), ((), ())), preferred_element_type=F32).astype(BF16)
    precond[...] = jnp.dot(third, ql[...], preferred_element_type=F32)

    value = precond[...]
    square = value * value
    tile = square[0:8]
    for r in range(8, nb, 8):
        tile = tile + square[r : r + 8]
    total = tile[:, 0:128]
    for k in range(128, value.shape[1], 128):
        total = total + tile[:, k : k + 128]
    mine[...] = total

    def exchange(phase, n, me, ident, slots):
        slots[me] = mine[...]

        def make(peer, at):
            return pltpu.make_async_remote_copy(
                src_ref=mine,
                dst_ref=slots.at[at],
                send_sem=ar_send.at[phase, peer],
                recv_sem=ar_recv.at[phase, at],
                device_id=ident(peer),
                device_id_type=MESH,
            )

        loop(1, n, lambda k: make(lax.rem(me + k, n), me).start())

        def wait(k):
            peer = lax.rem(me + k, n)
            make(peer, peer).wait_recv()

        loop(1, n, wait)
        loop(1, n, lambda k: make(lax.rem(me + k, n), me).wait_send())
        total = slots[0]
        for k in range(1, n):
            total = total + slots[k]
        mine[...] = total

    exchange(0, n_shard, shard_me, shard_id, all_shard)
    exchange(1, n_grp, grp_me, grp_id, all_grp)

    rms = jnp.sqrt(jnp.sum(mine[...], keepdims=True) / count + 1e-06)
    scale = jnp.minimum(jnp.float32(1.0), 1.1 / rms)
    out_ref[...] = (precond[...] * scale).astype(BF16)

    def drain(c):
        swap(c).wait_send()
        final(c).wait_send()
        for k in range(2):
            pl.when(goes_down(z))(lambda: piece(c, 0, k, z).wait_send())
            pl.when(goes_up(z))(lambda: piece(c, 1, k, z).wait_send())
            pl.when(z < planes - 1)(lambda: last(c, 0, k, part.at[c, 0, own]).wait_send())
            falls = (z == 0) | (bottom(z - 1, c) > 0)
            pl.when(falls)(lambda: last(c, 1, k, part.at[c, 0, own]).wait_send())

        def each(s):
            pl.when(goes_down(s) & (s != z))(lambda: down(c, s).wait_send())
            pl.when(goes_up(s) & (s != z))(lambda: up(c, s).wait_send())
            comes = (z < s) | ((z > s) & (bottom(s, c) > 0))
            near = (s == z + 1) | (s == down_z)
            pl.when(comes & jnp.logical_not(near))(lambda: back(c, s, part.at[c, s]).wait_send())

        loop(0, planes, each)

    loop(0, chunks, drain)

    def drain_factor(s):
        pl.when(relayed(s))(lambda: relay_first(s, relay_slot(s)).wait_send())
        pl.when(jnp.logical_not(relayed(s)))(lambda: factor(s).wait_send())

    def drain_relay(k):
        @pl.when(relays(k))
        def _():
            relay_second(k).wait_send()
            relay_third(k).wait_send()

    loop(z, planes, drain_factor)
    loop(0, 2, drain_relay)


def body(sizes, gradients, left_factor, right_factor):
    rows, nb = gradients.shape[1:]
    half = rows // 2
    chunks = half // LANES
    planes = PLANES
    n_shard, n_grp = 2 * planes, sizes[0] * sizes[1] * sizes[2]
    count = gradients.shape[0] * n_grp * rows * nb * n_shard
    dma = pltpu.SemaphoreType.DMA
    turned = pl.pallas_call(
        functools.partial(kernel, count, sizes),
        out_shape=jax.ShapeDtypeStruct((nb, rows), BF16),
        in_specs=[
            pl.BlockSpec(memory_space=pl.ANY),
            pl.BlockSpec(memory_space=pl.ANY),
            pl.BlockSpec(memory_space=pl.ANY),
        ],
        out_specs=pl.BlockSpec(memory_space=pltpu.VMEM),
        scratch_shapes=[
            pltpu.VMEM((planes, 2 * nb, half), BF16),
            pltpu.VMEM((chunks, planes, 2 * nb, LANES), BF16),
            pltpu.VMEM((chunks, planes, 2 * nb, LANES), BF16),
            pltpu.VMEM((planes, 2 * nb, 2 * nb), BF16),
            pltpu.VMEM((planes, 2 * nb, 2 * nb), BF16),
            pltpu.VMEM((rows, rows), BF16),
            pltpu.VMEM((2 * nb, half), BF16),
            pltpu.VMEM((2 * nb, half), F32),
            pltpu.VMEM((2, 2 * nb, half), F32),
            pltpu.VMEM((2 * chunks, nb, LANES), BF16),
            pltpu.VMEM((chunks, nb, LANES), F32),
            pltpu.VMEM((chunks, nb, LANES), F32),
            pltpu.VMEM((nb, half), F32),
            pltpu.VMEM((2, 2, chunks, nb, LANES), BF16),
            pltpu.VMEM((nb, half), BF16),
            pltpu.VMEM((2, nb, 2 * nb), BF16),
            pltpu.VMEM((2, nb, 2 * nb), BF16),
            pltpu.VMEM((nb, rows), F32),
            pltpu.VMEM((8, 128), F32),
            pltpu.VMEM((n_shard, 8, 128), F32),
            pltpu.VMEM((n_grp, 8, 128), F32),
            dma((chunks, planes)),
            dma((chunks, planes)),
            dma((chunks, planes)),
            dma((2, 2, chunks)),
            dma((2, 2, chunks)),
            dma((chunks, planes)),
            dma((chunks, planes)),
            dma((2, 2, chunks)),
            dma((2, 2, chunks)),
            dma((chunks,)),
            dma((chunks,)),
            dma((planes,)),
            dma((planes,)),
            dma((3, 2)),
            dma((2, 2)),
            dma((chunks,)),
            dma((chunks,)),
            dma((planes + 3,)),
            dma((2, max(n_shard, n_grp))),
            dma((2, max(n_shard, n_grp))),
        ],
        compiler_params=pltpu.CompilerParams(
            collective_id=0, has_side_effects=True, vmem_limit_bytes=67043328
        ),
        name="precondition",
    )(gradients[0].T, right_factor[0], left_factor[0])
    return turned.T[None]


def split_mesh(devices, sizes):
    return Mesh(devices.reshape(*sizes, PLANES, 2), GRP + SHARD)


def program(split, sizes):
    in_specs = (P(GRP, None, SHARD), P(GRP, None, None), P(GRP, SHARD, None))
    return jax.shard_map(
        functools.partial(body, sizes), mesh=split, in_specs=in_specs, out_specs=P(GRP, None, SHARD), check_vma=False
    )


def solution(mesh):
    sizes = (2, 4, 2)
    return program(split_mesh(mesh.devices, sizes), sizes)
```

```python
import functools

import jax
import jax.numpy as jnp
from jax import lax
from jax.experimental import pallas as pl
from jax.experimental.pallas import tpu as pltpu
from jax.sharding import Mesh
from jax.sharding import PartitionSpec as P

MESH = pl.DeviceIdType.MESH
SHARD = ("shard_0", "shard_1")
GRP = ("grp_0", "grp_1", "grp_2")
F32 = jnp.float32
BF16 = jnp.bfloat16

PLANES = 8
LANES = 128
HOPS = 4


def low(s, c, chunks):
    return jnp.where(s >= 5, s - 3, jnp.where((s == 4) & (c >= chunks // 2), 1, 0))


def loop(lower, upper, body):
    def step(i, carry):
        body(i)
        return carry

    lax.fori_loop(lower, upper, step, 0)


def kernel(
    count,
    sizes,
    g_ref,
    qr_hbm,
    ql_hbm,
    out_ref,
    gt,
    part,
    held,
    qr,
    qrt,
    ql,
    first,
    first_sum,
    share,
    second,
    leaving,
    coming,
    kept,
    landed,
    swapped,
    relay_in,
    relay_out,
    precond,
    mine,
    all_shard,
    all_grp,
    down_send,
    up_send,
    gather_recv,
    piece_send,
    piece_recv,
    back_send,
    back_recv,
    last_send,
    landed_recv,
    swap_send,
    swap_recv,
    factor_send,
    factor_recv,
    relay_send,
    relay_recv,
    final_send,
    final_recv,
    load_sem,
    chain_sem,
    ar_send,
    ar_recv,
):
    planes, chunks = PLANES, part.shape[0]
    nb, half = leaving.shape[1], first.shape[1]
    z, y = lax.axis_index("shard_0"), lax.axis_index("shard_1")
    g0, g1, g2 = lax.axis_index("grp_0"), lax.axis_index("grp_1"), lax.axis_index("grp_2")
    n1, n2 = sizes[1], sizes[2]
    n_shard, n_grp = planes * 2, sizes[0] * n1 * n2
    shard_me = z * 2 + y
    grp_me = (g0 * n1 + g1) * n2 + g2
    up_z, down_z = lax.rem(z + 1, planes), lax.rem(z + planes - 1, planes)
    own = pl.ds(pl.multiple_of(y * nb, 16), nb)
    other = pl.ds(pl.multiple_of((1 - y) * nb, 16), nb)

    def lanes(c, base=0):
        return pl.ds(pl.multiple_of(base + c * LANES, LANES), LANES)

    def shard_id(p):
        return {"shard_0": p // 2, "shard_1": lax.rem(p, 2)}

    def grp_id(p):
        return {"grp_0": p // (n1 * n2), "grp_1": lax.rem(p // n2, n1), "grp_2": lax.rem(p, n2)}

    def bottom(s, c):
        return low(s, c, chunks)

    def at_hop(h, body):
        s = z + h
        pl.when((s < planes) & (z >= bottom(s, 0)))(lambda: body(s, 0))

        @pl.when(h > 0)
        def _():
            t = lax.rem(z - h + planes, planes)
            pl.when((t > z) & (z < bottom(t, 0)))(lambda: body(t, 1))

    def load(s):
        columns = pl.ds(pl.multiple_of(s * 2 * nb, 128), 2 * nb)
        return pltpu.make_async_copy(qr_hbm.at[:, columns], qr.at[s, own], load_sem.at[s])

    load_ql = pltpu.make_async_copy(ql_hbm, ql, load_sem.at[planes])
    mine_half = pl.ds(pl.multiple_of(y * half, LANES), half)
    swap_half = pl.ds(pl.multiple_of((1 - y) * half, LANES), half)
    load_mine = pltpu.make_async_copy(g_ref.at[:, mine_half], gt.at[z, own], load_sem.at[planes + 1])
    load_swap = pltpu.make_async_copy(g_ref.at[:, swap_half], swapped, load_sem.at[planes + 2])
    load_swap.start()
    load_mine.start()
    loop(0, HOPS + 1, lambda h: at_hop(h, lambda s, k: load(s).start()))
    load_ql.start()

    barrier = pltpu.get_barrier_semaphore()

    def greet(semaphore, ids):
        for peer in ids:
            pl.semaphore_signal(semaphore, inc=1, device_id=peer, device_id_type=MESH)

    x_ids = [{"grp_1": lax.rem(g1 + k, n1)} for k in (1, n1 - 1)] if n1 > 1 else []
    y_ids = [{"shard_1": 1 - y}] + ([{"grp_0": 1 - g0, "shard_1": 1 - y}] if sizes[0] > 1 else [])
    core_ids = [{"grp_2": 1 - g2}] if n2 > 1 else []
    z_ids = [{"shard_0": to, "shard_1": line} for to in (up_z, down_z) for line in (y, 1 - y)]
    greet(barrier, y_ids + z_ids + x_ids + core_ids)
    load_swap.wait()
    load_mine.wait()
    pl.semaphore_wait(barrier, len(y_ids) + len(z_ids) + len(x_ids) + len(core_ids))

    chain = [y_ids, x_ids, x_ids, core_ids]

    def pass_on(k):
        if k > 0:
            pl.semaphore_wait(chain_sem.at[k - 1], len(chain[k - 1])) if chain[k - 1] else None
        if k < len(chain):
            greet(chain_sem.at[k], chain[k])

    pass_on(0)

    def remote(src, dst, send, recv, to_z, to_y):
        return pltpu.make_async_remote_copy(
            src_ref=src,
            dst_ref=dst,
            send_sem=send,
            recv_sem=recv,
            device_id={"shard_0": to_z, "shard_1": to_y},
            device_id_type=MESH,
        )

    def swap(c):
        return remote(swapped.at[:, lanes(c)], gt.at[z, own, lanes(c)], swap_send.at[c], swap_recv.at[c], z, 1 - y)

    def factor(s):
        ref = qr.at[s, own]
        return remote(ref, ref, factor_send.at[s], factor_recv.at[s], z, 1 - y)

    def down(c, s):
        ref = gt.at[s, :, lanes(c)]
        return remote(ref, ref, down_send.at[c, s], gather_recv.at[c, s], down_z, y)

    def up(c, s):
        ref = gt.at[s, :, lanes(c)]
        return remote(ref, ref, up_send.at[c, s], gather_recv.at[c, s], up_z, y)

    def back(c, s, src):
        rising = (z < s) & (z >= bottom(s, c))
        parent = jnp.where(rising, up_z, down_z)
        return remote(src, held.at[c, s], back_send.at[c, s], back_recv.at[c, s], parent, y)

    def last(c, way, k, src):
        to_z = (up_z, down_z)[way]
        send, recv = last_send.at[way, k, c], landed_recv.at[way, y, c]
        return remote(src, landed.at[way, y, c], send, recv, to_z, y if k == 0 else 1 - y)

    def start_last(c, way, ref):
        last(c, way, 0, ref.at[own]).start()
        last(c, way, 1, ref.at[other]).start()

    def final(c):
        return remote(leaving.at[c], coming.at[c], final_send.at[c], final_recv.at[c], z, 1 - y)

    def goes_down(s):
        return (z <= s) & (z - 1 >= bottom(s, 0))

    def goes_up(s):
        return ((z >= s) & (bottom(s, 0) > 0)) | ((z < s) & (z + 1 < bottom(s, 0)))

    def got_back(c, s):
        remote(held.at[c, s], held.at[c, s], back_send.at[0, 0], back_recv.at[c, s], up_z, y).wait_recv()

    def relayed(s):
        return ((z <= 2) & (s == z + 4)) | ((z == 0) & (s == 5))

    def relays(k):
        return (z == 7) | ((k == 0) & ((z == 2) | (z == 3)))

    def relay_slot(s):
        return jnp.where((z == 0) & (s == 4), 1, 0)

    def relay_first(s, k):
        via = jnp.where(z == 0, down_z, up_z)
        return remote(qr.at[s, own], relay_in.at[k], relay_send.at[0, k], relay_recv.at[0, k], via, y)

    def relay_second(k):
        return remote(relay_in.at[k], relay_out.at[k], relay_send.at[1, k], relay_recv.at[1, k], z, 1 - y)

    def relay_third(k):
        s = jnp.where(z == 7, 5 - k, z + 3)
        to = jnp.where(z == 7, up_z, down_z)
        return remote(relay_out.at[k], qr.at[s, other], relay_send.at[2, k], factor_recv.at[s], to, y)

    def start_relay(s, k):
        @pl.when(relayed(s))
        def _():
            load(s).wait()
            relay_first(s, relay_slot(s)).start()

    def send_factor(s, k):
        @pl.when(jnp.logical_not(relayed(s)))
        def _():
            load(s).wait()
            factor(s).start()

    def relay_on(k):
        @pl.when(relays(k))
        def _():
            relay_first(z, k).wait_recv()
            relay_second(k).start()

    def relay_home(k):
        @pl.when(relays(k))
        def _():
            relay_second(k).wait_recv()
            relay_third(k).start()

    def piece(c, way, k, s):
        ref = gt.at[s, own if k == 0 else other, lanes(c)]
        return remote(ref, ref, piece_send.at[way, k, c], piece_recv.at[way, k, c], (down_z, up_z)[way], y)

    def start_pieces(c, k):
        pl.when(goes_down(z))(lambda: piece(c, 0, k, z).start())
        pl.when(goes_up(z))(lambda: piece(c, 1, k, z).start())

    def inject(c):
        swap(c).wait_recv()
        start_pieces(c, 1)

    def gather_hop(h, arrive):
        def chunk(c):
            s = z + h

            @pl.when((s < planes) & (z >= bottom(s, 0)))
            def _():
                arrive(c, 0, s)
                pl.when(goes_down(s))(lambda: down(c, s).start())

            t = lax.rem(z - h + planes, planes)

            @pl.when(((z > t) & (bottom(t, 0) > 0)) | ((z < t) & (z < bottom(t, 0))))
            def _():
                arrive(c, 1, t)
                pl.when(goes_up(t))(lambda: up(c, t).start())

        loop(0, chunks, chunk)

    def arrive_pieces(c, way, s):
        piece(c, way, 0, s).wait_recv()
        piece(c, way, 1, s).wait_recv()

    def arrive_whole(c, way, s):
        down(c, s).wait_recv()

    def multiply_own(s, k):
        first_sum[own, :] += jnp.dot(qr[s, own, :], gt[s], preferred_element_type=F32)

    def multiply_other(s, k):
        factor(s).wait_recv()
        first_sum[other, :] += jnp.dot(qr[s, other, :], gt[s], preferred_element_type=F32)

    loop(0, chunks, lambda c: swap(c).start())
    at_hop(0, send_factor)
    loop(HOPS - 1, HOPS + 1, lambda h: at_hop(h, start_relay))
    loop(0, chunks, lambda c: start_pieces(c, 0))
    loop(0, chunks, inject)
    relay_on(0)
    loop(1, HOPS + 1, lambda h: at_hop(h, send_factor))
    pass_on(1)
    first_sum[...] = jnp.zeros_like(first_sum)
    gather_hop(1, arrive_pieces)
    relay_on(1)
    relay_home(0)
    pass_on(2)
    at_hop(0, multiply_own)
    at_hop(1, multiply_own)
    at_hop(0, multiply_other)

    def hop(h):
        gather_hop(h, arrive_whole)
        pl.when(h == 2)(lambda: relay_home(1))
        at_hop(h, multiply_own)
        at_hop(h - 1, multiply_other)

    loop(2, HOPS + 1, hop)
    at_hop(HOPS, multiply_other)
    first[...] = first_sum[...].astype(BF16)

    pass_on(3)

    def product(s, k):
        qrt[s] = qr[s].T
        share[k] = jnp.dot(qrt[s], first[...], preferred_element_type=F32)

    def contribute(c, s, k, send):
        floor = bottom(s, c)
        child = ((z >= floor) & (z - 1 >= floor)) | (z + 1 < floor)

        @pl.when(child)
        def _():
            got_back(c, s)
            part[c, s] = (share[k, :, lanes(c)] + held[c, s].astype(F32)).astype(BF16)

        @pl.when(jnp.logical_not(child))
        def _():
            part[c, s] = share[k, :, lanes(c)].astype(BF16)

        send(c, s, k, part.at[c, s])

    def back_phase(h, send):
        at_hop(h, product)

        def chunk(c):
            at_hop(h, lambda s, k: contribute(c, s, k, send))
            t = z - h

            @pl.when((t >= 0) & (bottom(t, c) > 0))
            def _():
                got_back(c, t)
                send(c, t, 1, held.at[c, t])

        loop(0, chunks, chunk)

    def send_back(c, s, k, ref):
        back(c, s, ref).start()

    def send_last(c, s, k, ref):
        start_last(c, k, ref)

    loop(0, HOPS - 2, lambda i: back_phase(HOPS - i, send_back))

    pass_on(4)

    product(z, 0)
    kept[...] = share[0, own, :]

    def leave(c):
        leaving[c] = share[0, other, lanes(c)]
        final(c).start()

    loop(0, chunks, leave)
    back_phase(2, send_back)
    back_phase(1, send_last)

    def arrived(way, line, c):
        return remote(
            landed.at[way, line, c],
            landed.at[way, line, c],
            last_send.at[0, 0, 0],
            landed_recv.at[way, line, c],
            up_z,
            y,
        )

    def finish(c):
        final(c).wait_recv()

        @pl.when(z > 0)
        def _():
            arrived(0, y, c).wait_recv()
            arrived(0, 1 - y, c).wait_recv()
            kept[:, lanes(c)] += landed[0, y, c].astype(F32)
            coming[c] += landed[0, 1 - y, c].astype(F32)

        @pl.when(bottom(z, c) > 0)
        def _():
            arrived(1, y, c).wait_recv()
            arrived(1, 1 - y, c).wait_recv()
            kept[:, lanes(c)] += landed[1, y, c].astype(F32)
            coming[c] += landed[1, 1 - y, c].astype(F32)

        second[y * chunks + c] = kept[:, lanes(c)].astype(BF16)
        second[(1 - y) * chunks + c] = coming[c].astype(BF16)

    loop(0, chunks, finish)

    load_ql.wait()
    sub = jnp.concatenate([second[c] for c in range(2 * chunks)], axis=1)
    third = lax.dot_general(sub, ql[...], (((1,), (1,)), ((), ())), preferred_element_type=F32).astype(BF16)
    precond[...] = jnp.dot(third, ql[...], preferred_element_type=F32)

    value = precond[...]
    square = value * value
    tile = square[0:8]
    for r in range(8, nb, 8):
        tile = tile + square[r : r + 8]
    total = tile[:, 0:128]
    for k in range(128, value.shape[1], 128):
        total = total + tile[:, k : k + 128]
    mine[...] = total

    def exchange(phase, n, me, ident, slots):
        slots[me] = mine[...]

        def make(peer, at):
            return pltpu.make_async_remote_copy(
                src_ref=mine,
                dst_ref=slots.at[at],
                send_sem=ar_send.at[phase, peer],
                recv_sem=ar_recv.at[phase, at],
                device_id=ident(peer),
                device_id_type=MESH,
            )

        loop(1, n, lambda k: make(lax.rem(me + k, n), me).start())

        def wait(k):
            peer = lax.rem(me + k, n)
            make(peer, peer).wait_recv()

        loop(1, n, wait)
        loop(1, n, lambda k: make(lax.rem(me + k, n), me).wait_send())
        total = slots[0]
        for k in range(1, n):
            total = total + slots[k]
        mine[...] = total

    exchange(0, n_shard, shard_me, shard_id, all_shard)
    exchange(1, n_grp, grp_me, grp_id, all_grp)

    rms = jnp.sqrt(jnp.sum(mine[...], keepdims=True) / count + 1e-06)
    scale = jnp.minimum(jnp.float32(1.0), 1.1 / rms)
    out_ref[...] = (precond[...] * scale).astype(BF16)

    def drain(c):
        swap(c).wait_send()
        final(c).wait_send()
        for k in range(2):
            pl.when(goes_down(z))(lambda: piece(c, 0, k, z).wait_send())
            pl.when(goes_up(z))(lambda: piece(c, 1, k, z).wait_send())
            pl.when(z < planes - 1)(lambda: last(c, 0, k, part.at[c, 0, own]).wait_send())
            falls = (z == 0) | (bottom(z - 1, c) > 0)
            pl.when(falls)(lambda: last(c, 1, k, part.at[c, 0, own]).wait_send())

        def each(s):
            pl.when(goes_down(s) & (s != z))(lambda: down(c, s).wait_send())
            pl.when(goes_up(s) & (s != z))(lambda: up(c, s).wait_send())
            comes = (z < s) | ((z > s) & (bottom(s, c) > 0))
            near = (s == z + 1) | (s == down_z)
            pl.when(comes & jnp.logical_not(near))(lambda: back(c, s, part.at[c, s]).wait_send())

        loop(0, planes, each)

    loop(0, chunks, drain)

    def drain_factor(s):
        pl.when(relayed(s))(lambda: relay_first(s, relay_slot(s)).wait_send())
        pl.when(jnp.logical_not(relayed(s)))(lambda: factor(s).wait_send())

    def drain_relay(k):
        @pl.when(relays(k))
        def _():
            relay_second(k).wait_send()
            relay_third(k).wait_send()

    loop(z, planes, drain_factor)
    loop(0, 2, drain_relay)


def body(sizes, gradients, left_factor, right_factor):
    rows, nb = gradients.shape[1:]
    half = rows // 2
    chunks = half // LANES
    planes = PLANES
    n_shard, n_grp = 2 * planes, sizes[0] * sizes[1] * sizes[2]
    count = gradients.shape[0] * n_grp * rows * nb * n_shard
    dma = pltpu.SemaphoreType.DMA
    turned = pl.pallas_call(
        functools.partial(kernel, count, sizes),
        out_shape=jax.ShapeDtypeStruct((nb, rows), BF16),
        in_specs=[
            pl.BlockSpec(memory_space=pl.ANY),
            pl.BlockSpec(memory_space=pl.ANY),
            pl.BlockSpec(memory_space=pl.ANY),
        ],
        out_specs=pl.BlockSpec(memory_space=pltpu.VMEM),
        scratch_shapes=[
            pltpu.VMEM((planes, 2 * nb, half), BF16),
            pltpu.VMEM((chunks, planes, 2 * nb, LANES), BF16),
            pltpu.VMEM((chunks, planes, 2 * nb, LANES), BF16),
            pltpu.VMEM((planes, 2 * nb, 2 * nb), BF16),
            pltpu.VMEM((planes, 2 * nb, 2 * nb), BF16),
            pltpu.VMEM((rows, rows), BF16),
            pltpu.VMEM((2 * nb, half), BF16),
            pltpu.VMEM((2 * nb, half), F32),
            pltpu.VMEM((2, 2 * nb, half), F32),
            pltpu.VMEM((2 * chunks, nb, LANES), BF16),
            pltpu.VMEM((chunks, nb, LANES), F32),
            pltpu.VMEM((chunks, nb, LANES), F32),
            pltpu.VMEM((nb, half), F32),
            pltpu.VMEM((2, 2, chunks, nb, LANES), BF16),
            pltpu.VMEM((nb, half), BF16),
            pltpu.VMEM((2, nb, 2 * nb), BF16),
            pltpu.VMEM((2, nb, 2 * nb), BF16),
            pltpu.VMEM((nb, rows), F32),
            pltpu.VMEM((8, 128), F32),
            pltpu.VMEM((n_shard, 8, 128), F32),
            pltpu.VMEM((n_grp, 8, 128), F32),
            dma((chunks, planes)),
            dma((chunks, planes)),
            dma((chunks, planes)),
            dma((2, 2, chunks)),
            dma((2, 2, chunks)),
            dma((chunks, planes)),
            dma((chunks, planes)),
            dma((2, 2, chunks)),
            dma((2, 2, chunks)),
            dma((chunks,)),
            dma((chunks,)),
            dma((planes,)),
            dma((planes,)),
            dma((3, 2)),
            dma((2, 2)),
            dma((chunks,)),
            dma((chunks,)),
            dma((planes + 3,)),
            pltpu.SemaphoreType.REGULAR((4,)),
            dma((2, max(n_shard, n_grp))),
            dma((2, max(n_shard, n_grp))),
        ],
        compiler_params=pltpu.CompilerParams(
            collective_id=0, has_side_effects=True, vmem_limit_bytes=67043328
        ),
        name="precondition",
    )(gradients[0].T, right_factor[0], left_factor[0])
    return turned.T[None]


def split_mesh(devices, sizes):
    return Mesh(devices.reshape(*sizes, PLANES, 2), GRP + SHARD)


def program(split, sizes):
    in_specs = (P(GRP, None, SHARD), P(GRP, None, None), P(GRP, SHARD, None))
    return jax.shard_map(
        functools.partial(body, sizes), mesh=split, in_specs=in_specs, out_specs=P(GRP, None, SHARD), check_vma=False
    )


def solution(mesh):
    sizes = (2, 4, 2)
    return program(split_mesh(mesh.devices, sizes), sizes)
```

```python
import functools

import jax
import jax.numpy as jnp
from jax import lax
from jax.experimental import pallas as pl
from jax.experimental.pallas import tpu as pltpu
from jax.sharding import Mesh
from jax.sharding import PartitionSpec as P

MESH = pl.DeviceIdType.MESH
SHARD = ("shard_0", "shard_1")
GRP = ("grp_0", "grp_1", "grp_2")
F32 = jnp.float32
BF16 = jnp.bfloat16

PLANES = 8
LANES = 128
HOPS = 4


def low(s, c, chunks):
    return jnp.where(s >= 5, s - 3, jnp.where((s == 4) & (c >= chunks // 2), 1, 0))


def loop(lower, upper, body):
    def step(i, carry):
        body(i)
        return carry

    lax.fori_loop(lower, upper, step, 0)


def kernel(
    count,
    sizes,
    g_ref,
    qr_hbm,
    ql_hbm,
    out_ref,
    gt,
    part,
    held,
    qr,
    qrt,
    ql,
    first,
    first_sum,
    share,
    second,
    leaving,
    coming,
    kept,
    landed,
    swapped,
    relay_in,
    relay_out,
    precond,
    mine,
    all_shard,
    all_grp,
    down_send,
    up_send,
    gather_recv,
    piece_send,
    piece_recv,
    back_send,
    back_recv,
    last_send,
    landed_recv,
    swap_send,
    swap_recv,
    factor_send,
    factor_recv,
    relay_send,
    relay_recv,
    final_send,
    final_recv,
    load_sem,
    chain_sem,
    ar_send,
    ar_recv,
):
    planes, chunks = PLANES, part.shape[0]
    nb, half = leaving.shape[1], first.shape[1]
    z, y = lax.axis_index("shard_0"), lax.axis_index("shard_1")
    g0, g1, g2 = lax.axis_index("grp_0"), lax.axis_index("grp_1"), lax.axis_index("grp_2")
    n1, n2 = sizes[1], sizes[2]
    n_shard, n_grp = planes * 2, sizes[0] * n1 * n2
    shard_me = z * 2 + y
    grp_me = (g0 * n1 + g1) * n2 + g2
    up_z, down_z = lax.rem(z + 1, planes), lax.rem(z + planes - 1, planes)
    own = pl.ds(pl.multiple_of(y * nb, 16), nb)
    other = pl.ds(pl.multiple_of((1 - y) * nb, 16), nb)

    def lanes(c, base=0):
        return pl.ds(pl.multiple_of(base + c * LANES, LANES), LANES)

    def shard_id(p):
        return {"shard_0": p // 2, "shard_1": lax.rem(p, 2)}

    def grp_id(p):
        return {"grp_0": p // (n1 * n2), "grp_1": lax.rem(p // n2, n1), "grp_2": lax.rem(p, n2)}

    def bottom(s, c):
        return low(s, c, chunks)

    def at_hop(h, body):
        s = z + h
        pl.when((s < planes) & (z >= bottom(s, 0)))(lambda: body(s, 0))

        @pl.when(h > 0)
        def _():
            t = lax.rem(z - h + planes, planes)
            pl.when((t > z) & (z < bottom(t, 0)))(lambda: body(t, 1))

    def load(s):
        columns = pl.ds(pl.multiple_of(s * 2 * nb, 128), 2 * nb)
        return pltpu.make_async_copy(qr_hbm.at[:, columns], qr.at[s, own], load_sem.at[s])

    load_ql = pltpu.make_async_copy(ql_hbm, ql, load_sem.at[planes])
    mine_half = pl.ds(pl.multiple_of(y * half, LANES), half)
    swap_half = pl.ds(pl.multiple_of((1 - y) * half, LANES), half)
    load_mine = pltpu.make_async_copy(g_ref.at[:, mine_half], gt.at[z, own], load_sem.at[planes + 1])
    load_swap = pltpu.make_async_copy(g_ref.at[:, swap_half], swapped, load_sem.at[planes + 2])
    load_swap.start()
    load_mine.start()
    loop(0, HOPS + 1, lambda h: at_hop(h, lambda s, k: load(s).start()))
    load_ql.start()

    barrier = pltpu.get_barrier_semaphore()

    def greet(semaphore, ids):
        for peer in ids:
            pl.semaphore_signal(semaphore, inc=1, device_id=peer, device_id_type=MESH)

    x_ids = [{"grp_1": lax.rem(g1 + k, n1)} for k in (1, n1 - 1)] if n1 > 1 else []
    y_ids = [{"shard_1": 1 - y}] + ([{"grp_0": 1 - g0, "shard_1": 1 - y}] if sizes[0] > 1 else [])
    core_ids = [{"grp_2": 1 - g2}] if n2 > 1 else []
    z_ids = [{"shard_0": to, "shard_1": line} for to in (up_z, down_z) for line in (y, 1 - y)]
    greet(barrier, y_ids + z_ids + x_ids + core_ids)
    load_swap.wait()
    load_mine.wait()
    pl.semaphore_wait(barrier, len(y_ids) + len(z_ids) + len(x_ids) + len(core_ids))

    chain = [y_ids, x_ids, x_ids, core_ids]

    def pass_on(k):
        if k > 0:
            pl.semaphore_wait(chain_sem.at[k - 1], len(chain[k - 1])) if chain[k - 1] else None
        if k < len(chain):
            greet(chain_sem.at[k], chain[k])

    pass_on(0)

    def remote(src, dst, send, recv, to_z, to_y):
        return pltpu.make_async_remote_copy(
            src_ref=src,
            dst_ref=dst,
            send_sem=send,
            recv_sem=recv,
            device_id={"shard_0": to_z, "shard_1": to_y},
            device_id_type=MESH,
        )

    def swap(c):
        return remote(swapped.at[:, lanes(c)], gt.at[z, own, lanes(c)], swap_send.at[c], swap_recv.at[c], z, 1 - y)

    def factor(s):
        ref = qr.at[s, own]
        return remote(ref, ref, factor_send.at[s], factor_recv.at[s], z, 1 - y)

    def down(c, s):
        ref = gt.at[s, :, lanes(c)]
        return remote(ref, ref, down_send.at[c, s], gather_recv.at[c, s], down_z, y)

    def up(c, s):
        ref = gt.at[s, :, lanes(c)]
        return remote(ref, ref, up_send.at[c, s], gather_recv.at[c, s], up_z, y)

    def back(c, s, src):
        rising = (z < s) & (z >= bottom(s, c))
        parent = jnp.where(rising, up_z, down_z)
        return remote(src, held.at[c, s], back_send.at[c, s], back_recv.at[c, s], parent, y)

    def last(c, way, k, src):
        to_z = (up_z, down_z)[way]
        send, recv = last_send.at[way, k, c], landed_recv.at[way, y, c]
        return remote(src, landed.at[way, y, c], send, recv, to_z, y if k == 0 else 1 - y)

    def start_last(c, way, ref):
        last(c, way, 0, ref.at[own]).start()
        last(c, way, 1, ref.at[other]).start()

    def final(c):
        return remote(leaving.at[c], coming.at[c], final_send.at[c], final_recv.at[c], z, 1 - y)

    def goes_down(s):
        return (z <= s) & (z - 1 >= bottom(s, 0))

    def goes_up(s):
        return ((z >= s) & (bottom(s, 0) > 0)) | ((z < s) & (z + 1 < bottom(s, 0)))

    def got_back(c, s):
        remote(held.at[c, s], held.at[c, s], back_send.at[0, 0], back_recv.at[c, s], up_z, y).wait_recv()

    def relayed(s):
        return ((z <= 2) & (s == z + 4)) | ((z == 0) & (s == 5))

    def relays(k):
        return (z == 7) | ((k == 0) & ((z == 2) | (z == 3)))

    def relay_slot(s):
        return jnp.where((z == 0) & (s == 4), 1, 0)

    def relay_first(s, k):
        via = jnp.where(z == 0, down_z, up_z)
        return remote(qr.at[s, own], relay_in.at[k], relay_send.at[0, k], relay_recv.at[0, k], via, y)

    def relay_second(k):
        return remote(relay_in.at[k], relay_out.at[k], relay_send.at[1, k], relay_recv.at[1, k], z, 1 - y)

    def relay_third(k):
        s = jnp.where(z == 7, 5 - k, z + 3)
        to = jnp.where(z == 7, up_z, down_z)
        return remote(relay_out.at[k], qr.at[s, other], relay_send.at[2, k], factor_recv.at[s], to, y)

    def start_relay(s, k):
        @pl.when(relayed(s))
        def _():
            load(s).wait()
            relay_first(s, relay_slot(s)).start()

    def send_factor(s, k):
        @pl.when(jnp.logical_not(relayed(s)))
        def _():
            load(s).wait()
            factor(s).start()

    def relay_on(k):
        @pl.when(relays(k))
        def _():
            relay_first(z, k).wait_recv()
            relay_second(k).start()

    def relay_home(k):
        @pl.when(relays(k))
        def _():
            relay_second(k).wait_recv()
            relay_third(k).start()

    def piece(c, way, k, s):
        ref = gt.at[s, own if k == 0 else other, lanes(c)]
        return remote(ref, ref, piece_send.at[way, k, c], piece_recv.at[way, k, c], (down_z, up_z)[way], y)

    def start_pieces(c, k):
        pl.when(goes_down(z))(lambda: piece(c, 0, k, z).start())
        pl.when(goes_up(z))(lambda: piece(c, 1, k, z).start())

    def inject(c):
        swap(c).wait_recv()
        start_pieces(c, 1)

    def gather_hop(h, arrive):
        def chunk(c):
            s = z + h

            @pl.when((s < planes) & (z >= bottom(s, 0)))
            def _():
                arrive(c, 0, s)
                pl.when(goes_down(s))(lambda: down(c, s).start())

            t = lax.rem(z - h + planes, planes)

            @pl.when(((z > t) & (bottom(t, 0) > 0)) | ((z < t) & (z < bottom(t, 0))))
            def _():
                arrive(c, 1, t)
                pl.when(goes_up(t))(lambda: up(c, t).start())

        loop(0, chunks, chunk)

    def arrive_pieces(c, way, s):
        piece(c, way, 0, s).wait_recv()
        piece(c, way, 1, s).wait_recv()

    def arrive_whole(c, way, s):
        down(c, s).wait_recv()

    def multiply_own(s, k):
        first_sum[own, :] += jnp.dot(qr[s, own, :], gt[s], preferred_element_type=F32)

    def multiply_other(s, k):
        factor(s).wait_recv()
        first_sum[other, :] += jnp.dot(qr[s, other, :], gt[s], preferred_element_type=F32)

    loop(0, chunks, lambda c: swap(c).start())
    at_hop(0, send_factor)
    loop(HOPS - 1, HOPS + 1, lambda h: at_hop(h, start_relay))
    loop(0, chunks, lambda c: start_pieces(c, 0))
    loop(0, chunks, inject)
    relay_on(0)
    loop(1, HOPS + 1, lambda h: at_hop(h, send_factor))
    pass_on(1)
    first_sum[...] = jnp.zeros_like(first_sum)
    gather_hop(1, arrive_pieces)
    relay_on(1)
    relay_home(0)
    pass_on(2)
    at_hop(0, multiply_own)
    at_hop(1, multiply_own)
    at_hop(0, multiply_other)

    def hop(h):
        gather_hop(h, arrive_whole)
        pl.when(h == 2)(lambda: relay_home(1))
        at_hop(h, multiply_own)
        at_hop(h - 1, multiply_other)

    loop(2, HOPS + 1, hop)
    at_hop(HOPS, multiply_other)
    first[...] = first_sum[...].astype(BF16)

    pass_on(3)

    def product(s, k):
        qrt[s] = qr[s].T
        share[k] = jnp.dot(qrt[s], first[...], preferred_element_type=F32)

    def contribute(c, s, k, send):
        floor = bottom(s, c)
        child = ((z >= floor) & (z - 1 >= floor)) | (z + 1 < floor)

        @pl.when(child)
        def _():
            got_back(c, s)
            part[c, s] = (share[k, :, lanes(c)] + held[c, s].astype(F32)).astype(BF16)

        @pl.when(jnp.logical_not(child))
        def _():
            part[c, s] = share[k, :, lanes(c)].astype(BF16)

        send(c, s, k, part.at[c, s])

    def back_phase(h, send):
        at_hop(h, product)

        def chunk(c):
            at_hop(h, lambda s, k: contribute(c, s, k, send))
            t = z - h

            @pl.when((t >= 0) & (bottom(t, c) > 0))
            def _():
                got_back(c, t)
                send(c, t, 1, held.at[c, t])

        loop(0, chunks, chunk)

    def send_back(c, s, k, ref):
        back(c, s, ref).start()

    def send_last(c, s, k, ref):
        start_last(c, k, ref)

    loop(0, HOPS - 2, lambda i: back_phase(HOPS - i, send_back))

    pass_on(4)

    product(z, 0)
    kept[...] = share[0, own, :]

    def leave(c):
        leaving[c] = share[0, other, lanes(c)]
        final(c).start()

    loop(0, chunks, leave)
    back_phase(2, send_back)
    back_phase(1, send_last)

    def arrived(way, line, c):
        return remote(
            landed.at[way, line, c],
            landed.at[way, line, c],
            last_send.at[0, 0, 0],
            landed_recv.at[way, line, c],
            up_z,
            y,
        )

    def finish(c):
        final(c).wait_recv()

        @pl.when(z > 0)
        def _():
            arrived(0, y, c).wait_recv()
            arrived(0, 1 - y, c).wait_recv()
            kept[:, lanes(c)] += landed[0, y, c].astype(F32)
            coming[c] += landed[0, 1 - y, c].astype(F32)

        @pl.when(bottom(z, c) > 0)
        def _():
            arrived(1, y, c).wait_recv()
            arrived(1, 1 - y, c).wait_recv()
            kept[:, lanes(c)] += landed[1, y, c].astype(F32)
            coming[c] += landed[1, 1 - y, c].astype(F32)

        second[y * chunks + c] = kept[:, lanes(c)].astype(BF16)
        second[(1 - y) * chunks + c] = coming[c].astype(BF16)

    loop(0, chunks, finish)

    load_ql.wait()
    sub = jnp.concatenate([second[c] for c in range(2 * chunks)], axis=1)
    third = lax.dot_general(sub, ql[...], (((1,), (1,)), ((), ())), preferred_element_type=F32).astype(BF16)
    precond[...] = jnp.dot(third, ql[...], preferred_element_type=F32)

    value = precond[...]
    square = value * value
    tile = square[0:8]
    for r in range(8, nb, 8):
        tile = tile + square[r : r + 8]
    total = tile[:, 0:128]
    for k in range(128, value.shape[1], 128):
        total = total + tile[:, k : k + 128]
    mine[...] = total

    def exchange(phase, n, me, ident, slots):
        slots[me] = mine[...]

        def make(peer, at):
            return pltpu.make_async_remote_copy(
                src_ref=mine,
                dst_ref=slots.at[at],
                send_sem=ar_send.at[phase, peer],
                recv_sem=ar_recv.at[phase, at],
                device_id=ident(peer),
                device_id_type=MESH,
            )

        loop(1, n, lambda k: make(lax.rem(me + k, n), me).start())

        def wait(k):
            peer = lax.rem(me + k, n)
            make(peer, peer).wait_recv()

        loop(1, n, wait)
        loop(1, n, lambda k: make(lax.rem(me + k, n), me).wait_send())
        total = slots[0]
        for k in range(1, n):
            total = total + slots[k]
        mine[...] = total

    exchange(0, n_shard, shard_me, shard_id, all_shard)
    exchange(1, n_grp, grp_me, grp_id, all_grp)

    rms = jnp.sqrt(jnp.sum(mine[...], keepdims=True) / count + 1e-06)
    scale = jnp.minimum(jnp.float32(1.0), 1.1 / rms)
    out_ref[...] = (precond[...] * scale).astype(BF16)

    def drain(c):
        swap(c).wait_send()
        final(c).wait_send()
        for k in range(2):
            pl.when(goes_down(z))(lambda: piece(c, 0, k, z).wait_send())
            pl.when(goes_up(z))(lambda: piece(c, 1, k, z).wait_send())
            pl.when(z < planes - 1)(lambda: last(c, 0, k, part.at[c, 0, own]).wait_send())
            falls = (z == 0) | (bottom(z - 1, c) > 0)
            pl.when(falls)(lambda: last(c, 1, k, part.at[c, 0, own]).wait_send())

        def each(s):
            pl.when(goes_down(s) & (s != z))(lambda: down(c, s).wait_send())
            pl.when(goes_up(s) & (s != z))(lambda: up(c, s).wait_send())
            comes = (z < s) | ((z > s) & (bottom(s, c) > 0))
            near = (s == z + 1) | (s == down_z)
            pl.when(comes & jnp.logical_not(near))(lambda: back(c, s, part.at[c, s]).wait_send())

        loop(0, planes, each)

    loop(0, chunks, drain)

    def drain_factor(s):
        pl.when(relayed(s))(lambda: relay_first(s, relay_slot(s)).wait_send())
        pl.when(jnp.logical_not(relayed(s)))(lambda: factor(s).wait_send())

    def drain_relay(k):
        @pl.when(relays(k))
        def _():
            relay_second(k).wait_send()
            relay_third(k).wait_send()

    loop(z, planes, drain_factor)
    loop(0, 2, drain_relay)


def body(sizes, gradients, left_factor, right_factor):
    rows, nb = gradients.shape[1:]
    half = rows // 2
    chunks = half // LANES
    planes = PLANES
    n_shard, n_grp = 2 * planes, sizes[0] * sizes[1] * sizes[2]
    count = gradients.shape[0] * n_grp * rows * nb * n_shard
    dma = pltpu.SemaphoreType.DMA
    turned = pl.pallas_call(
        functools.partial(kernel, count, sizes),
        out_shape=jax.ShapeDtypeStruct((nb, rows), BF16),
        in_specs=[
            pl.BlockSpec(memory_space=pl.ANY),
            pl.BlockSpec(memory_space=pl.ANY),
            pl.BlockSpec(memory_space=pl.ANY),
        ],
        out_specs=pl.BlockSpec(memory_space=pltpu.VMEM),
        scratch_shapes=[
            pltpu.VMEM((planes, 2 * nb, half), BF16),
            pltpu.VMEM((chunks, planes, 2 * nb, LANES), BF16),
            pltpu.VMEM((chunks, planes, 2 * nb, LANES), BF16),
            pltpu.VMEM((planes, 2 * nb, 2 * nb), BF16),
            pltpu.VMEM((planes, 2 * nb, 2 * nb), BF16),
            pltpu.VMEM((rows, rows), BF16),
            pltpu.VMEM((2 * nb, half), BF16),
            pltpu.VMEM((2 * nb, half), F32),
            pltpu.VMEM((2, 2 * nb, half), F32),
            pltpu.VMEM((2 * chunks, nb, LANES), BF16),
            pltpu.VMEM((chunks, nb, LANES), F32),
            pltpu.VMEM((chunks, nb, LANES), F32),
            pltpu.VMEM((nb, half), F32),
            pltpu.VMEM((2, 2, chunks, nb, LANES), BF16),
            pltpu.VMEM((nb, half), BF16),
            pltpu.VMEM((2, nb, 2 * nb), BF16),
            pltpu.VMEM((2, nb, 2 * nb), BF16),
            pltpu.VMEM((nb, rows), F32),
            pltpu.VMEM((8, 128), F32),
            pltpu.VMEM((n_shard, 8, 128), F32),
            pltpu.VMEM((n_grp, 8, 128), F32),
            dma((chunks, planes)),
            dma((chunks, planes)),
            dma((chunks, planes)),
            dma((2, 2, chunks)),
            dma((2, 2, chunks)),
            dma((chunks, planes)),
            dma((chunks, planes)),
            dma((2, 2, chunks)),
            dma((2, 2, chunks)),
            dma((chunks,)),
            dma((chunks,)),
            dma((planes,)),
            dma((planes,)),
            dma((3, 2)),
            dma((2, 2)),
            dma((chunks,)),
            dma((chunks,)),
            dma((planes + 3,)),
            pltpu.SemaphoreType.REGULAR((4,)),
            dma((2, max(n_shard, n_grp))),
            dma((2, max(n_shard, n_grp))),
        ],
        compiler_params=pltpu.CompilerParams(
            collective_id=0, has_side_effects=True, vmem_limit_bytes=55500000
        ),
        name="precondition",
    )(gradients[0].T, right_factor[0], left_factor[0])
    return turned.T[None]


def split_mesh(devices, sizes):
    return Mesh(devices.reshape(*sizes, PLANES, 2), GRP + SHARD)


def program(split, sizes):
    in_specs = (P(GRP, None, SHARD), P(GRP, None, None), P(GRP, SHARD, None))
    return jax.shard_map(
        functools.partial(body, sizes), mesh=split, in_specs=in_specs, out_specs=P(GRP, None, SHARD), check_vma=False
    )


def solution(mesh):
    sizes = (2, 4, 2)
    return program(split_mesh(mesh.devices, sizes), sizes)
```

```python
import functools

import jax
import jax.numpy as jnp
from jax import lax
from jax.experimental import pallas as pl
from jax.experimental.pallas import tpu as pltpu
from jax.sharding import Mesh
from jax.sharding import PartitionSpec as P

MESH = pl.DeviceIdType.MESH
SHARD = ("shard_0", "shard_1")
GRP = ("grp_0", "grp_1", "grp_2")
F32 = jnp.float32
BF16 = jnp.bfloat16

PLANES = 8
LANES = 128
HOPS = 4


def low(s, c, chunks):
    return jnp.where(s >= 5, s - 3, jnp.where((s == 4) & (c >= chunks // 2), 1, 0))


def loop(lower, upper, body):
    def step(i, carry):
        body(i)
        return carry

    lax.fori_loop(lower, upper, step, 0)


def kernel(
    count,
    sizes,
    g_ref,
    qr_hbm,
    ql_hbm,
    out_ref,
    gt,
    part,
    held,
    qr,
    qrt,
    ql,
    first,
    first_sum,
    share,
    second,
    leaving,
    coming,
    kept,
    landed,
    swapped,
    relay_in,
    relay_out,
    precond,
    mine,
    all_shard,
    all_grp,
    down_send,
    up_send,
    gather_recv,
    piece_send,
    piece_recv,
    back_send,
    back_recv,
    last_send,
    landed_recv,
    swap_send,
    swap_recv,
    factor_send,
    factor_recv,
    relay_send,
    relay_recv,
    final_send,
    final_recv,
    load_sem,
    chain_sem,
    turn_sem,
    ar_send,
    ar_recv,
):
    planes, chunks = PLANES, part.shape[0]
    nb, half = leaving.shape[1], first.shape[1]
    z, y = lax.axis_index("shard_0"), lax.axis_index("shard_1")
    g0, g1, g2 = lax.axis_index("grp_0"), lax.axis_index("grp_1"), lax.axis_index("grp_2")
    n1, n2 = sizes[1], sizes[2]
    n_shard, n_grp = planes * 2, sizes[0] * n1 * n2
    shard_me = z * 2 + y
    grp_me = (g0 * n1 + g1) * n2 + g2
    up_z, down_z = lax.rem(z + 1, planes), lax.rem(z + planes - 1, planes)
    own = pl.ds(pl.multiple_of(y * nb, 16), nb)
    other = pl.ds(pl.multiple_of((1 - y) * nb, 16), nb)

    def lanes(c, base=0):
        return pl.ds(pl.multiple_of(base + c * LANES, LANES), LANES)

    def shard_id(p):
        return {"shard_0": p // 2, "shard_1": lax.rem(p, 2)}

    def grp_id(p):
        return {"grp_0": p // (n1 * n2), "grp_1": lax.rem(p // n2, n1), "grp_2": lax.rem(p, n2)}

    def bottom(s, c):
        return low(s, c, chunks)

    def at_hop(h, body):
        s = z + h
        pl.when((s < planes) & (z >= bottom(s, 0)))(lambda: body(s, 0))

        @pl.when(h > 0)
        def _():
            t = lax.rem(z - h + planes, planes)
            pl.when((t > z) & (z < bottom(t, 0)))(lambda: body(t, 1))

    def load(s):
        columns = pl.ds(pl.multiple_of(s * 2 * nb, 128), 2 * nb)
        return pltpu.make_async_copy(qr_hbm.at[:, columns], qr.at[s, own], load_sem.at[s])

    load_ql = pltpu.make_async_copy(ql_hbm, ql, load_sem.at[planes])
    mine_half = pl.ds(pl.multiple_of(y * half, LANES), half)
    swap_half = pl.ds(pl.multiple_of((1 - y) * half, LANES), half)
    load_mine = pltpu.make_async_copy(g_ref.at[:, mine_half], gt.at[z, own], load_sem.at[planes + 1])
    load_swap = pltpu.make_async_copy(g_ref.at[:, swap_half], swapped, load_sem.at[planes + 2])
    load_swap.start()
    load_mine.start()
    loop(0, HOPS + 1, lambda h: at_hop(h, lambda s, k: load(s).start()))
    load_ql.start()

    barrier = pltpu.get_barrier_semaphore()

    def greet(semaphore, ids):
        for peer in ids:
            pl.semaphore_signal(semaphore, inc=1, device_id=peer, device_id_type=MESH)

    x_ids = [{"grp_1": lax.rem(g1 + k, n1)} for k in (1, n1 - 1)] if n1 > 1 else []
    y_ids = [{"shard_1": 1 - y}] + ([{"grp_0": 1 - g0, "shard_1": 1 - y}] if sizes[0] > 1 else [])
    core_ids = [{"grp_2": 1 - g2}] if n2 > 1 else []
    z_ids = [{"shard_0": to, "shard_1": line} for to in (up_z, down_z) for line in (y, 1 - y)]
    greet(barrier, y_ids + z_ids + x_ids + core_ids)
    load_swap.wait()
    load_mine.wait()
    pl.semaphore_wait(barrier, len(y_ids) + len(z_ids) + len(x_ids) + len(core_ids))

    chain = [y_ids, x_ids, x_ids, core_ids]

    def pass_on(k):
        if k > 0:
            pl.semaphore_wait(chain_sem.at[k - 1], len(chain[k - 1])) if chain[k - 1] else None
        if k < len(chain):
            greet(chain_sem.at[k], chain[k])

    pass_on(0)

    def remote(src, dst, send, recv, to_z, to_y):
        return pltpu.make_async_remote_copy(
            src_ref=src,
            dst_ref=dst,
            send_sem=send,
            recv_sem=recv,
            device_id={"shard_0": to_z, "shard_1": to_y},
            device_id_type=MESH,
        )

    def swap(c):
        return remote(swapped.at[:, lanes(c)], gt.at[z, own, lanes(c)], swap_send.at[c], swap_recv.at[c], z, 1 - y)

    def factor(s):
        ref = qr.at[s, own]
        return remote(ref, ref, factor_send.at[s], factor_recv.at[s], z, 1 - y)

    def down(c, s):
        ref = gt.at[s, :, lanes(c)]
        return remote(ref, ref, down_send.at[c, s], gather_recv.at[c, s], down_z, y)

    def up(c, s):
        ref = gt.at[s, :, lanes(c)]
        return remote(ref, ref, up_send.at[c, s], gather_recv.at[c, s], up_z, y)

    def back(c, s, src):
        rising = (z < s) & (z >= bottom(s, c))
        parent = jnp.where(rising, up_z, down_z)
        return remote(src, held.at[c, s], back_send.at[c, s], back_recv.at[c, s], parent, y)

    def last(c, way, k, src):
        to_z = (up_z, down_z)[way]
        send, recv = last_send.at[way, k, c], landed_recv.at[way, y, c]
        return remote(src, landed.at[way, y, c], send, recv, to_z, y if k == 0 else 1 - y)

    def start_last(c, way, ref):
        last(c, way, 0, ref.at[own]).start()
        last(c, way, 1, ref.at[other]).start()

    def final(c):
        return remote(leaving.at[c], coming.at[c], final_send.at[c], final_recv.at[c], z, 1 - y)

    def goes_down(s):
        return (z <= s) & (z - 1 >= bottom(s, 0))

    def goes_up(s):
        return ((z >= s) & (bottom(s, 0) > 0)) | ((z < s) & (z + 1 < bottom(s, 0)))

    def got_back(c, s):
        remote(held.at[c, s], held.at[c, s], back_send.at[0, 0], back_recv.at[c, s], up_z, y).wait_recv()

    def relayed(s):
        return ((z <= 2) & (s == z + 4)) | ((z == 0) & (s == 5))

    def relays(k):
        return (z == 7) | ((k == 0) & ((z == 2) | (z == 3)))

    def relay_slot(s):
        return jnp.where((z == 0) & (s == 4), 1, 0)

    def relay_first(s, k):
        via = jnp.where(z == 0, down_z, up_z)
        return remote(qr.at[s, own], relay_in.at[k], relay_send.at[0, k], relay_recv.at[0, k], via, y)

    def relay_second(k):
        return remote(relay_in.at[k], relay_out.at[k], relay_send.at[1, k], relay_recv.at[1, k], z, 1 - y)

    def relay_third(k):
        s = jnp.where(z == 7, 5 - k, z + 3)
        to = jnp.where(z == 7, up_z, down_z)
        return remote(relay_out.at[k], qr.at[s, other], relay_send.at[2, k], factor_recv.at[s], to, y)

    def start_relay(s, k):
        @pl.when(relayed(s))
        def _():
            load(s).wait()
            relay_first(s, relay_slot(s)).start()

    def send_factor(s, k):
        @pl.when(jnp.logical_not(relayed(s)))
        def _():
            load(s).wait()
            factor(s).start()

    def relay_on(k):
        @pl.when(relays(k))
        def _():
            relay_first(z, k).wait_recv()
            relay_second(k).start()

    def relay_home(k):
        @pl.when(relays(k))
        def _():
            relay_second(k).wait_recv()
            relay_third(k).start()

    def piece(c, way, k, s):
        ref = gt.at[s, own if k == 0 else other, lanes(c)]
        return remote(ref, ref, piece_send.at[way, k, c], piece_recv.at[way, k, c], (down_z, up_z)[way], y)

    def start_pieces(c, k):
        pl.when(goes_down(z))(lambda: piece(c, 0, k, z).start())
        pl.when(goes_up(z))(lambda: piece(c, 1, k, z).start())

    def inject(c):
        swap(c).wait_recv()
        start_pieces(c, 1)

    def gather_hop(h, arrive):
        def chunk(c):
            s = z + h

            @pl.when((s < planes) & (z >= bottom(s, 0)))
            def _():
                arrive(c, 0, s)
                pl.when(goes_down(s))(lambda: down(c, s).start())

            t = lax.rem(z - h + planes, planes)

            @pl.when(((z > t) & (bottom(t, 0) > 0)) | ((z < t) & (z < bottom(t, 0))))
            def _():
                arrive(c, 1, t)
                pl.when(goes_up(t))(lambda: up(c, t).start())

        loop(0, chunks, chunk)

    def arrive_pieces(c, way, s):
        piece(c, way, 0, s).wait_recv()
        piece(c, way, 1, s).wait_recv()

    def arrive_whole(c, way, s):
        down(c, s).wait_recv()

    def multiply_own(s, k):
        first_sum[own, :] += jnp.dot(qr[s, own, :], gt[s], preferred_element_type=F32)

    def multiply_other(s, k):
        factor(s).wait_recv()
        first_sum[other, :] += jnp.dot(qr[s, other, :], gt[s], preferred_element_type=F32)

    if n2 > 1:
        @pl.when(g2 == 1)
        def _():
            pl.semaphore_wait(turn_sem, 1)

    def let_go():
        if n2 > 1:
            @pl.when(g2 == 0)
            def _():
                pl.semaphore_signal(turn_sem, inc=1, device_id={"grp_2": 1 - g2}, device_id_type=MESH)

    loop(0, chunks, lambda c: swap(c).start())
    at_hop(0, send_factor)
    loop(HOPS - 1, HOPS + 1, lambda h: at_hop(h, start_relay))
    loop(0, chunks, lambda c: start_pieces(c, 0))
    loop(0, chunks, inject)
    relay_on(0)
    loop(1, HOPS + 1, lambda h: at_hop(h, send_factor))
    pass_on(1)
    first_sum[...] = jnp.zeros_like(first_sum)
    gather_hop(1, arrive_pieces)
    relay_on(1)
    relay_home(0)
    pass_on(2)
    at_hop(0, multiply_own)
    at_hop(1, multiply_own)
    at_hop(0, multiply_other)

    def hop(h):
        gather_hop(h, arrive_whole)
        pl.when(h == 2)(let_go)
        pl.when(h == 2)(lambda: relay_home(1))
        at_hop(h, multiply_own)
        at_hop(h - 1, multiply_other)

    loop(2, HOPS + 1, hop)
    pass_on(3)
    at_hop(HOPS, multiply_other)
    first[...] = first_sum[...].astype(BF16)

    def product(s, k):
        qrt[s] = qr[s].T
        share[k] = jnp.dot(qrt[s], first[...], preferred_element_type=F32)

    def contribute(c, s, k, send):
        floor = bottom(s, c)
        child = ((z >= floor) & (z - 1 >= floor)) | (z + 1 < floor)

        @pl.when(child)
        def _():
            got_back(c, s)
            part[c, s] = (share[k, :, lanes(c)] + held[c, s].astype(F32)).astype(BF16)

        @pl.when(jnp.logical_not(child))
        def _():
            part[c, s] = share[k, :, lanes(c)].astype(BF16)

        send(c, s, k, part.at[c, s])

    def back_phase(h, send):
        at_hop(h, product)

        def chunk(c):
            at_hop(h, lambda s, k: contribute(c, s, k, send))
            t = z - h

            @pl.when((t >= 0) & (bottom(t, c) > 0))
            def _():
                got_back(c, t)
                send(c, t, 1, held.at[c, t])

        loop(0, chunks, chunk)

    def send_back(c, s, k, ref):
        back(c, s, ref).start()

    def send_last(c, s, k, ref):
        start_last(c, k, ref)

    loop(0, HOPS - 2, lambda i: back_phase(HOPS - i, send_back))

    product(z, 0)
    kept[...] = share[0, own, :]

    def leave(c):
        leaving[c] = share[0, other, lanes(c)]
        final(c).start()

    loop(0, chunks, leave)
    back_phase(2, send_back)
    back_phase(1, send_last)

    def arrived(way, line, c):
        return remote(
            landed.at[way, line, c],
            landed.at[way, line, c],
            last_send.at[0, 0, 0],
            landed_recv.at[way, line, c],
            up_z,
            y,
        )

    def finish(c):
        final(c).wait_recv()

        @pl.when(z > 0)
        def _():
            arrived(0, y, c).wait_recv()
            arrived(0, 1 - y, c).wait_recv()
            kept[:, lanes(c)] += landed[0, y, c].astype(F32)
            coming[c] += landed[0, 1 - y, c].astype(F32)

        @pl.when(bottom(z, c) > 0)
        def _():
            arrived(1, y, c).wait_recv()
            arrived(1, 1 - y, c).wait_recv()
            kept[:, lanes(c)] += landed[1, y, c].astype(F32)
            coming[c] += landed[1, 1 - y, c].astype(F32)

        second[y * chunks + c] = kept[:, lanes(c)].astype(BF16)
        second[(1 - y) * chunks + c] = coming[c].astype(BF16)

    loop(0, chunks, finish)

    load_ql.wait()
    sub = jnp.concatenate([second[c] for c in range(2 * chunks)], axis=1)
    third = lax.dot_general(sub, ql[...], (((1,), (1,)), ((), ())), preferred_element_type=F32).astype(BF16)
    precond[...] = jnp.dot(third, ql[...], preferred_element_type=F32)

    value = precond[...]
    square = value * value
    tile = square[0:8]
    for r in range(8, nb, 8):
        tile = tile + square[r : r + 8]
    total = tile[:, 0:128]
    for k in range(128, value.shape[1], 128):
        total = total + tile[:, k : k + 128]
    mine[...] = jnp.sum(total, axis=0, keepdims=True)

    def exchange(phase, n, me, ident, slots):
        slots[me] = mine[...]

        def make(peer, at):
            return pltpu.make_async_remote_copy(
                src_ref=mine,
                dst_ref=slots.at[at],
                send_sem=ar_send.at[phase, peer],
                recv_sem=ar_recv.at[phase, at],
                device_id=ident(peer),
                device_id_type=MESH,
            )

        loop(1, n, lambda k: make(lax.rem(me + k, n), me).start())

        def wait(k):
            peer = lax.rem(me + k, n)
            make(peer, peer).wait_recv()

        loop(1, n, wait)
        loop(1, n, lambda k: make(lax.rem(me + k, n), me).wait_send())
        total = slots[0]
        for k in range(1, n):
            total = total + slots[k]
        mine[...] = total

    pass_on(4)
    exchange(0, n_shard, shard_me, shard_id, all_shard)
    exchange(1, n_grp, grp_me, grp_id, all_grp)

    rms = jnp.sqrt(jnp.sum(mine[...], keepdims=True) / count + 1e-06)
    scale = jnp.minimum(jnp.float32(1.0), 1.1 / rms)
    out_ref[...] = (precond[...] * scale).astype(BF16)

    def drain(c):
        swap(c).wait_send()
        final(c).wait_send()
        for k in range(2):
            pl.when(goes_down(z))(lambda: piece(c, 0, k, z).wait_send())
            pl.when(goes_up(z))(lambda: piece(c, 1, k, z).wait_send())
            pl.when(z < planes - 1)(lambda: last(c, 0, k, part.at[c, 0, own]).wait_send())
            falls = (z == 0) | (bottom(z - 1, c) > 0)
            pl.when(falls)(lambda: last(c, 1, k, part.at[c, 0, own]).wait_send())

        def each(s):
            pl.when(goes_down(s) & (s != z))(lambda: down(c, s).wait_send())
            pl.when(goes_up(s) & (s != z))(lambda: up(c, s).wait_send())
            comes = (z < s) | ((z > s) & (bottom(s, c) > 0))
            near = (s == z + 1) | (s == down_z)
            pl.when(comes & jnp.logical_not(near))(lambda: back(c, s, part.at[c, s]).wait_send())

        loop(0, planes, each)

    loop(0, chunks, drain)

    def drain_factor(s):
        pl.when(relayed(s))(lambda: relay_first(s, relay_slot(s)).wait_send())
        pl.when(jnp.logical_not(relayed(s)))(lambda: factor(s).wait_send())

    def drain_relay(k):
        @pl.when(relays(k))
        def _():
            relay_second(k).wait_send()
            relay_third(k).wait_send()

    loop(z, planes, drain_factor)
    loop(0, 2, drain_relay)


def body(sizes, gradients, left_factor, right_factor):
    rows, nb = gradients.shape[1:]
    half = rows // 2
    chunks = half // LANES
    planes = PLANES
    n_shard, n_grp = 2 * planes, sizes[0] * sizes[1] * sizes[2]
    count = gradients.shape[0] * n_grp * rows * nb * n_shard
    dma = pltpu.SemaphoreType.DMA
    turned = pl.pallas_call(
        functools.partial(kernel, count, sizes),
        out_shape=jax.ShapeDtypeStruct((nb, rows), BF16),
        in_specs=[
            pl.BlockSpec(memory_space=pl.ANY),
            pl.BlockSpec(memory_space=pl.ANY),
            pl.BlockSpec(memory_space=pl.ANY),
        ],
        out_specs=pl.BlockSpec(memory_space=pltpu.VMEM),
        scratch_shapes=[
            pltpu.VMEM((planes, 2 * nb, half), BF16),
            pltpu.VMEM((chunks, planes, 2 * nb, LANES), BF16),
            pltpu.VMEM((chunks, planes, 2 * nb, LANES), BF16),
            pltpu.VMEM((planes, 2 * nb, 2 * nb), BF16),
            pltpu.VMEM((planes, 2 * nb, 2 * nb), BF16),
            pltpu.VMEM((rows, rows), BF16),
            pltpu.VMEM((2 * nb, half), BF16),
            pltpu.VMEM((2 * nb, half), F32),
            pltpu.VMEM((2, 2 * nb, half), F32),
            pltpu.VMEM((2 * chunks, nb, LANES), BF16),
            pltpu.VMEM((chunks, nb, LANES), F32),
            pltpu.VMEM((chunks, nb, LANES), F32),
            pltpu.VMEM((nb, half), F32),
            pltpu.VMEM((2, 2, chunks, nb, LANES), BF16),
            pltpu.VMEM((nb, half), BF16),
            pltpu.VMEM((2, nb, 2 * nb), BF16),
            pltpu.VMEM((2, nb, 2 * nb), BF16),
            pltpu.VMEM((nb, rows), F32),
            pltpu.VMEM((1, 128), F32),
            pltpu.VMEM((n_shard, 1, 128), F32),
            pltpu.VMEM((n_grp, 1, 128), F32),
            dma((chunks, planes)),
            dma((chunks, planes)),
            dma((chunks, planes)),
            dma((2, 2, chunks)),
            dma((2, 2, chunks)),
            dma((chunks, planes)),
            dma((chunks, planes)),
            dma((2, 2, chunks)),
            dma((2, 2, chunks)),
            dma((chunks,)),
            dma((chunks,)),
            dma((planes,)),
            dma((planes,)),
            dma((3, 2)),
            dma((2, 2)),
            dma((chunks,)),
            dma((chunks,)),
            dma((planes + 3,)),
            pltpu.SemaphoreType.REGULAR((4,)),
            pltpu.SemaphoreType.REGULAR,
            dma((2, max(n_shard, n_grp))),
            dma((2, max(n_shard, n_grp))),
        ],
        compiler_params=pltpu.CompilerParams(
            collective_id=0, has_side_effects=True, vmem_limit_bytes=55500000
        ),
        name="precondition",
    )(gradients[0].T, right_factor[0], left_factor[0])
    return turned.T[None]


def split_mesh(devices, sizes):
    return Mesh(devices.reshape(*sizes, PLANES, 2), GRP + SHARD)


def program(split, sizes):
    in_specs = (P(GRP, None, SHARD), P(GRP, None, None), P(GRP, SHARD, None))
    return jax.shard_map(
        functools.partial(body, sizes), mesh=split, in_specs=in_specs, out_specs=P(GRP, None, SHARD), check_vma=False
    )


def solution(mesh):
    sizes = (2, 4, 2)
    return program(split_mesh(mesh.devices, sizes), sizes)
```

```python
import functools

import jax
import jax.numpy as jnp
from jax import lax
from jax.experimental import pallas as pl
from jax.experimental.pallas import tpu as pltpu
from jax.sharding import Mesh
from jax.sharding import PartitionSpec as P

MESH = pl.DeviceIdType.MESH
SHARD = ("shard_0", "shard_1")
GRP = ("grp_0", "grp_1", "grp_2")
F32 = jnp.float32
BF16 = jnp.bfloat16

PLANES = 8
LANES = 128
HOPS = 4


def low(s, c, chunks):
    return jnp.where(s >= 5, s - 3, jnp.where((s == 4) & (c >= chunks // 2), 1, 0))


def loop(lower, upper, body):
    def step(i, carry):
        body(i)
        return carry

    lax.fori_loop(lower, upper, step, 0)


def kernel(
    count,
    sizes,
    g_ref,
    qr_hbm,
    ql_hbm,
    out_ref,
    gt,
    part,
    held,
    qr,
    qrt,
    ql,
    first,
    first_sum,
    share,
    second,
    leaving,
    coming,
    kept,
    landed,
    swapped,
    relay_in,
    relay_out,
    precond,
    mine,
    all_shard,
    all_grp,
    down_send,
    up_send,
    gather_recv,
    piece_send,
    piece_recv,
    back_send,
    back_recv,
    last_send,
    landed_recv,
    swap_send,
    swap_recv,
    factor_send,
    factor_recv,
    relay_send,
    relay_recv,
    final_send,
    final_recv,
    load_sem,
    chain_sem,
    turn_sem,
    ar_send,
    ar_recv,
):
    planes, chunks = PLANES, part.shape[0]
    nb, half = leaving.shape[1], first.shape[1]
    z, y = lax.axis_index("shard_0"), lax.axis_index("shard_1")
    g0, g1, g2 = lax.axis_index("grp_0"), lax.axis_index("grp_1"), lax.axis_index("grp_2")
    n1, n2 = sizes[1], sizes[2]
    n_shard, n_grp = planes * 2, sizes[0] * n1 * n2
    shard_me = z * 2 + y
    grp_me = (g0 * n1 + g1) * n2 + g2
    up_z, down_z = lax.rem(z + 1, planes), lax.rem(z + planes - 1, planes)
    own = pl.ds(pl.multiple_of(y * nb, 16), nb)
    other = pl.ds(pl.multiple_of((1 - y) * nb, 16), nb)

    def lanes(c, base=0):
        return pl.ds(pl.multiple_of(base + c * LANES, LANES), LANES)

    def shard_id(p):
        return {"shard_0": p // 2, "shard_1": lax.rem(p, 2)}

    def grp_id(p):
        return {"grp_0": p // (n1 * n2), "grp_1": lax.rem(p // n2, n1), "grp_2": lax.rem(p, n2)}

    def bottom(s, c):
        return low(s, c, chunks)

    def at_hop(h, body):
        s = z + h
        pl.when((s < planes) & (z >= bottom(s, 0)))(lambda: body(s, 0))

        @pl.when(h > 0)
        def _():
            t = lax.rem(z - h + planes, planes)
            pl.when((t > z) & (z < bottom(t, 0)))(lambda: body(t, 1))

    def load(s):
        columns = pl.ds(pl.multiple_of(s * 2 * nb, 128), 2 * nb)
        return pltpu.make_async_copy(qr_hbm.at[:, columns], qr.at[s, own], load_sem.at[s])

    load_ql = pltpu.make_async_copy(ql_hbm, ql, load_sem.at[planes])
    mine_half = pl.ds(pl.multiple_of(y * half, LANES), half)
    swap_half = pl.ds(pl.multiple_of((1 - y) * half, LANES), half)
    load_mine = pltpu.make_async_copy(g_ref.at[:, mine_half], gt.at[z, own], load_sem.at[planes + 1])
    load_swap = pltpu.make_async_copy(g_ref.at[:, swap_half], swapped, load_sem.at[planes + 2])
    load_swap.start()
    load_mine.start()
    loop(0, HOPS + 1, lambda h: at_hop(h, lambda s, k: load(s).start()))
    load_ql.start()

    barrier = pltpu.get_barrier_semaphore()

    def greet(semaphore, ids):
        for peer in ids:
            pl.semaphore_signal(semaphore, inc=1, device_id=peer, device_id_type=MESH)

    x_ids = [{"grp_1": lax.rem(g1 + k, n1)} for k in (1, n1 - 1)] if n1 > 1 else []
    y_ids = [{"shard_1": 1 - y}] + ([{"grp_0": 1 - g0, "shard_1": 1 - y}] if sizes[0] > 1 else [])
    core_ids = [{"grp_2": 1 - g2}] if n2 > 1 else []
    z_ids = [{"shard_0": to, "shard_1": line} for to in (up_z, down_z) for line in (y, 1 - y)]
    greet(barrier, y_ids + z_ids + x_ids + core_ids)
    load_swap.wait()
    load_mine.wait()
    pl.semaphore_wait(barrier, len(y_ids) + len(z_ids) + len(x_ids) + len(core_ids))

    chain = [y_ids, x_ids, x_ids, core_ids]

    def pass_on(k):
        if k > 0:
            pl.semaphore_wait(chain_sem.at[k - 1], len(chain[k - 1])) if chain[k - 1] else None
        if k < len(chain):
            greet(chain_sem.at[k], chain[k])

    pass_on(0)

    def remote(src, dst, send, recv, to_z, to_y):
        return pltpu.make_async_remote_copy(
            src_ref=src,
            dst_ref=dst,
            send_sem=send,
            recv_sem=recv,
            device_id={"shard_0": to_z, "shard_1": to_y},
            device_id_type=MESH,
        )

    def swap(c):
        return remote(swapped.at[:, lanes(c)], gt.at[z, own, lanes(c)], swap_send.at[c], swap_recv.at[c], z, 1 - y)

    def factor(s):
        ref = qr.at[s, own]
        return remote(ref, ref, factor_send.at[s], factor_recv.at[s], z, 1 - y)

    def down(c, s):
        ref = gt.at[s, :, lanes(c)]
        return remote(ref, ref, down_send.at[c, s], gather_recv.at[c, s], down_z, y)

    def up(c, s):
        ref = gt.at[s, :, lanes(c)]
        return remote(ref, ref, up_send.at[c, s], gather_recv.at[c, s], up_z, y)

    def back(c, s, src):
        rising = (z < s) & (z >= bottom(s, c))
        parent = jnp.where(rising, up_z, down_z)
        return remote(src, held.at[c, s], back_send.at[c, s], back_recv.at[c, s], parent, y)

    def last(c, way, k, src):
        to_z = (up_z, down_z)[way]
        send, recv = last_send.at[way, k, c], landed_recv.at[way, y, c]
        return remote(src, landed.at[way, y, c], send, recv, to_z, y if k == 0 else 1 - y)

    def start_last(c, way, ref):
        last(c, way, 0, ref.at[own]).start()
        last(c, way, 1, ref.at[other]).start()

    def final(c):
        return remote(leaving.at[c], coming.at[c], final_send.at[c], final_recv.at[c], z, 1 - y)

    def goes_down(s):
        return (z <= s) & (z - 1 >= bottom(s, 0))

    def goes_up(s):
        return ((z >= s) & (bottom(s, 0) > 0)) | ((z < s) & (z + 1 < bottom(s, 0)))

    def got_back(c, s):
        remote(held.at[c, s], held.at[c, s], back_send.at[0, 0], back_recv.at[c, s], up_z, y).wait_recv()

    def relayed(s):
        return (z == 0) & ((s == 4) | (s == 5))

    def relays(k):
        return (z == 7) & (k >= 0)

    def relay_slot(s):
        return jnp.where((z == 0) & (s == 4), 1, 0)

    def relay_first(s, k):
        via = jnp.where(z == 0, down_z, up_z)
        return remote(qr.at[s, own], relay_in.at[k], relay_send.at[0, k], relay_recv.at[0, k], via, y)

    def relay_second(k):
        return remote(relay_in.at[k], relay_out.at[k], relay_send.at[1, k], relay_recv.at[1, k], z, 1 - y)

    def relay_third(k):
        s = jnp.where(z == 7, 5 - k, z + 3)
        to = jnp.where(z == 7, up_z, down_z)
        return remote(relay_out.at[k], qr.at[s, other], relay_send.at[2, k], factor_recv.at[s], to, y)

    def start_relay(s, k):
        @pl.when(relayed(s))
        def _():
            load(s).wait()
            relay_first(s, relay_slot(s)).start()

    def send_factor(s, k):
        @pl.when(jnp.logical_not(relayed(s)))
        def _():
            load(s).wait()
            factor(s).start()

    def relay_on(k):
        @pl.when(relays(k))
        def _():
            relay_first(z, k).wait_recv()
            relay_second(k).start()

    def relay_home(k):
        @pl.when(relays(k))
        def _():
            relay_second(k).wait_recv()
            relay_third(k).start()

    def piece(c, way, k, s):
        ref = gt.at[s, own if k == 0 else other, lanes(c)]
        return remote(ref, ref, piece_send.at[way, k, c], piece_recv.at[way, k, c], (down_z, up_z)[way], y)

    def start_pieces(c, k):
        pl.when(goes_down(z))(lambda: piece(c, 0, k, z).start())
        pl.when(goes_up(z))(lambda: piece(c, 1, k, z).start())

    def inject(c):
        swap(c).wait_recv()
        start_pieces(c, 1)

    def gather_hop(h, arrive):
        def chunk(c):
            s = z + h

            @pl.when((s < planes) & (z >= bottom(s, 0)))
            def _():
                arrive(c, 0, s)
                pl.when(goes_down(s))(lambda: down(c, s).start())

            t = lax.rem(z - h + planes, planes)

            @pl.when(((z > t) & (bottom(t, 0) > 0)) | ((z < t) & (z < bottom(t, 0))))
            def _():
                arrive(c, 1, t)
                pl.when(goes_up(t))(lambda: up(c, t).start())

        loop(0, chunks, chunk)

    def arrive_pieces(c, way, s):
        piece(c, way, 0, s).wait_recv()
        piece(c, way, 1, s).wait_recv()

    def arrive_whole(c, way, s):
        down(c, s).wait_recv()

    def multiply_own(s, k):
        first_sum[own, :] += jnp.dot(qr[s, own, :], gt[s], preferred_element_type=F32)

    def multiply_other(s, k):
        factor(s).wait_recv()
        first_sum[other, :] += jnp.dot(qr[s, other, :], gt[s], preferred_element_type=F32)

    if n2 > 1:
        @pl.when(g2 == 1)
        def _():
            pl.semaphore_wait(turn_sem, 1)

    def let_go():
        if n2 > 1:
            @pl.when(g2 == 0)
            def _():
                pl.semaphore_signal(turn_sem, inc=1, device_id={"grp_2": 1 - g2}, device_id_type=MESH)

    loop(0, chunks, lambda c: swap(c).start())
    at_hop(0, send_factor)
    loop(HOPS - 1, HOPS + 1, lambda h: at_hop(h, start_relay))
    loop(0, chunks, lambda c: start_pieces(c, 0))
    loop(0, chunks, inject)
    relay_on(0)
    loop(1, HOPS + 1, lambda h: at_hop(h, send_factor))
    pass_on(1)
    first_sum[...] = jnp.zeros_like(first_sum)
    gather_hop(1, arrive_pieces)
    relay_on(1)
    relay_home(0)
    pass_on(2)
    at_hop(0, multiply_own)
    at_hop(1, multiply_own)
    at_hop(0, multiply_other)

    def hop(h):
        gather_hop(h, arrive_whole)
        pl.when(h == 2)(let_go)
        pl.when(h == 2)(lambda: relay_home(1))
        at_hop(h, multiply_own)
        at_hop(h - 1, multiply_other)

    loop(2, HOPS + 1, hop)
    pass_on(3)
    at_hop(HOPS, multiply_other)
    first[...] = first_sum[...].astype(BF16)

    def product(s, k):
        qrt[s] = qr[s].T
        share[k] = jnp.dot(qrt[s], first[...], preferred_element_type=F32)

    def contribute(c, s, k, send):
        floor = bottom(s, c)
        child = ((z >= floor) & (z - 1 >= floor)) | (z + 1 < floor)

        @pl.when(child)
        def _():
            got_back(c, s)
            part[c, s] = (share[k, :, lanes(c)] + held[c, s].astype(F32)).astype(BF16)

        @pl.when(jnp.logical_not(child))
        def _():
            part[c, s] = share[k, :, lanes(c)].astype(BF16)

        send(c, s, k, part.at[c, s])

    def back_phase(h, send):
        at_hop(h, product)

        def chunk(c):
            at_hop(h, lambda s, k: contribute(c, s, k, send))
            t = z - h

            @pl.when((t >= 0) & (bottom(t, c) > 0))
            def _():
                got_back(c, t)
                send(c, t, 1, held.at[c, t])

        loop(0, chunks, chunk)

    def send_back(c, s, k, ref):
        back(c, s, ref).start()

    def send_last(c, s, k, ref):
        start_last(c, k, ref)

    loop(0, HOPS - 2, lambda i: back_phase(HOPS - i, send_back))

    product(z, 0)
    kept[...] = share[0, own, :]

    def leave(c):
        leaving[c] = share[0, other, lanes(c)]
        final(c).start()

    loop(0, chunks, leave)
    back_phase(2, send_back)
    back_phase(1, send_last)

    def arrived(way, line, c):
        return remote(
            landed.at[way, line, c],
            landed.at[way, line, c],
            last_send.at[0, 0, 0],
            landed_recv.at[way, line, c],
            up_z,
            y,
        )

    def finish(c):
        final(c).wait_recv()

        @pl.when(z > 0)
        def _():
            arrived(0, y, c).wait_recv()
            arrived(0, 1 - y, c).wait_recv()
            kept[:, lanes(c)] += landed[0, y, c].astype(F32)
            coming[c] += landed[0, 1 - y, c].astype(F32)

        @pl.when(bottom(z, c) > 0)
        def _():
            arrived(1, y, c).wait_recv()
            arrived(1, 1 - y, c).wait_recv()
            kept[:, lanes(c)] += landed[1, y, c].astype(F32)
            coming[c] += landed[1, 1 - y, c].astype(F32)

        second[y * chunks + c] = kept[:, lanes(c)].astype(BF16)
        second[(1 - y) * chunks + c] = coming[c].astype(BF16)

    loop(0, chunks, finish)

    load_ql.wait()
    sub = jnp.concatenate([second[c] for c in range(2 * chunks)], axis=1)
    third = lax.dot_general(sub, ql[...], (((1,), (1,)), ((), ())), preferred_element_type=F32).astype(BF16)
    precond[...] = jnp.dot(third, ql[...], preferred_element_type=F32)

    value = precond[...]
    square = value * value
    tile = square[0:8]
    for r in range(8, nb, 8):
        tile = tile + square[r : r + 8]
    total = tile[:, 0:128]
    for k in range(128, value.shape[1], 128):
        total = total + tile[:, k : k + 128]
    mine[...] = jnp.sum(total, axis=0, keepdims=True)

    def exchange(phase, n, me, ident, slots):
        slots[me] = mine[...]

        def make(peer, at):
            return pltpu.make_async_remote_copy(
                src_ref=mine,
                dst_ref=slots.at[at],
                send_sem=ar_send.at[phase, peer],
                recv_sem=ar_recv.at[phase, at],
                device_id=ident(peer),
                device_id_type=MESH,
            )

        loop(1, n, lambda k: make(lax.rem(me + k, n), me).start())

        def wait(k):
            peer = lax.rem(me + k, n)
            make(peer, peer).wait_recv()

        loop(1, n, wait)
        loop(1, n, lambda k: make(lax.rem(me + k, n), me).wait_send())
        total = slots[0]
        for k in range(1, n):
            total = total + slots[k]
        mine[...] = total

    pass_on(4)
    exchange(0, n_shard, shard_me, shard_id, all_shard)
    exchange(1, n_grp, grp_me, grp_id, all_grp)

    rms = jnp.sqrt(jnp.sum(mine[...], keepdims=True) / count + 1e-06)
    scale = jnp.minimum(jnp.float32(1.0), 1.1 / rms)
    out_ref[...] = (precond[...] * scale).astype(BF16)

    def drain(c):
        swap(c).wait_send()
        final(c).wait_send()
        for k in range(2):
            pl.when(goes_down(z))(lambda: piece(c, 0, k, z).wait_send())
            pl.when(goes_up(z))(lambda: piece(c, 1, k, z).wait_send())
            pl.when(z < planes - 1)(lambda: last(c, 0, k, part.at[c, 0, own]).wait_send())
            falls = (z == 0) | (bottom(z - 1, c) > 0)
            pl.when(falls)(lambda: last(c, 1, k, part.at[c, 0, own]).wait_send())

        def each(s):
            pl.when(goes_down(s) & (s != z))(lambda: down(c, s).wait_send())
            pl.when(goes_up(s) & (s != z))(lambda: up(c, s).wait_send())
            comes = (z < s) | ((z > s) & (bottom(s, c) > 0))
            near = (s == z + 1) | (s == down_z)
            pl.when(comes & jnp.logical_not(near))(lambda: back(c, s, part.at[c, s]).wait_send())

        loop(0, planes, each)

    loop(0, chunks, drain)

    def drain_factor(s):
        pl.when(relayed(s))(lambda: relay_first(s, relay_slot(s)).wait_send())
        pl.when(jnp.logical_not(relayed(s)))(lambda: factor(s).wait_send())

    def drain_relay(k):
        @pl.when(relays(k))
        def _():
            relay_second(k).wait_send()
            relay_third(k).wait_send()

    loop(z, planes, drain_factor)
    loop(0, 2, drain_relay)


def body(sizes, gradients, left_factor, right_factor):
    rows, nb = gradients.shape[1:]
    half = rows // 2
    chunks = half // LANES
    planes = PLANES
    n_shard, n_grp = 2 * planes, sizes[0] * sizes[1] * sizes[2]
    count = gradients.shape[0] * n_grp * rows * nb * n_shard
    dma = pltpu.SemaphoreType.DMA
    turned = pl.pallas_call(
        functools.partial(kernel, count, sizes),
        out_shape=jax.ShapeDtypeStruct((nb, rows), BF16),
        in_specs=[
            pl.BlockSpec(memory_space=pl.ANY),
            pl.BlockSpec(memory_space=pl.ANY),
            pl.BlockSpec(memory_space=pl.ANY),
        ],
        out_specs=pl.BlockSpec(memory_space=pltpu.VMEM),
        scratch_shapes=[
            pltpu.VMEM((planes, 2 * nb, half), BF16),
            pltpu.VMEM((chunks, planes, 2 * nb, LANES), BF16),
            pltpu.VMEM((chunks, planes, 2 * nb, LANES), BF16),
            pltpu.VMEM((planes, 2 * nb, 2 * nb), BF16),
            pltpu.VMEM((planes, 2 * nb, 2 * nb), BF16),
            pltpu.VMEM((rows, rows), BF16),
            pltpu.VMEM((2 * nb, half), BF16),
            pltpu.VMEM((2 * nb, half), F32),
            pltpu.VMEM((2, 2 * nb, half), F32),
            pltpu.VMEM((2 * chunks, nb, LANES), BF16),
            pltpu.VMEM((chunks, nb, LANES), F32),
            pltpu.VMEM((chunks, nb, LANES), F32),
            pltpu.VMEM((nb, half), F32),
            pltpu.VMEM((2, 2, chunks, nb, LANES), BF16),
            pltpu.VMEM((nb, half), BF16),
            pltpu.VMEM((2, nb, 2 * nb), BF16),
            pltpu.VMEM((2, nb, 2 * nb), BF16),
            pltpu.VMEM((nb, rows), F32),
            pltpu.VMEM((1, 128), F32),
            pltpu.VMEM((n_shard, 1, 128), F32),
            pltpu.VMEM((n_grp, 1, 128), F32),
            dma((chunks, planes)),
            dma((chunks, planes)),
            dma((chunks, planes)),
            dma((2, 2, chunks)),
            dma((2, 2, chunks)),
            dma((chunks, planes)),
            dma((chunks, planes)),
            dma((2, 2, chunks)),
            dma((2, 2, chunks)),
            dma((chunks,)),
            dma((chunks,)),
            dma((planes,)),
            dma((planes,)),
            dma((3, 2)),
            dma((2, 2)),
            dma((chunks,)),
            dma((chunks,)),
            dma((planes + 3,)),
            pltpu.SemaphoreType.REGULAR((4,)),
            pltpu.SemaphoreType.REGULAR,
            dma((2, max(n_shard, n_grp))),
            dma((2, max(n_shard, n_grp))),
        ],
        compiler_params=pltpu.CompilerParams(
            collective_id=0, has_side_effects=True, vmem_limit_bytes=55500000
        ),
        name="precondition",
    )(gradients[0].T, right_factor[0], left_factor[0])
    return turned.T[None]


def split_mesh(devices, sizes):
    return Mesh(devices.reshape(*sizes, PLANES, 2), GRP + SHARD)


def program(split, sizes):
    in_specs = (P(GRP, None, SHARD), P(GRP, None, None), P(GRP, SHARD, None))
    return jax.shard_map(
        functools.partial(body, sizes), mesh=split, in_specs=in_specs, out_specs=P(GRP, None, SHARD), check_vma=False
    )


def solution(mesh):
    sizes = (2, 4, 2)
    return program(split_mesh(mesh.devices, sizes), sizes)
```

```python
import functools

import jax
import jax.numpy as jnp
from jax import lax
from jax.experimental import pallas as pl
from jax.experimental.pallas import tpu as pltpu
from jax.sharding import Mesh
from jax.sharding import PartitionSpec as P

MESH = pl.DeviceIdType.MESH
SHARD = ("shard_0", "shard_1")
GRP = ("grp_0", "grp_1", "grp_2")
F32 = jnp.float32
BF16 = jnp.bfloat16

PLANES = 8
LANES = 128
HOPS = 4


def low(s, c, chunks):
    return jnp.where(s >= 5, s - 3, jnp.where((s == 4) & (c >= chunks // 2), 1, 0))


def loop(lower, upper, body):
    def step(i, carry):
        body(i)
        return carry

    lax.fori_loop(lower, upper, step, 0)


def kernel(
    count,
    sizes,
    g_ref,
    qr_hbm,
    ql_hbm,
    out_ref,
    gt,
    part,
    held,
    qr,
    qrt,
    ql,
    first,
    first_sum,
    share,
    second,
    leaving,
    coming,
    kept,
    landed,
    swapped,
    relay_in,
    relay_out,
    precond,
    mine,
    all_shard,
    all_grp,
    down_send,
    up_send,
    gather_recv,
    piece_send,
    piece_recv,
    back_send,
    back_recv,
    last_send,
    landed_recv,
    swap_send,
    swap_recv,
    factor_send,
    factor_recv,
    relay_send,
    relay_recv,
    final_send,
    final_recv,
    load_sem,
    chain_sem,
    turn_sem,
    ar_send,
    ar_recv,
):
    planes, chunks = PLANES, part.shape[0]
    nb, half = leaving.shape[1], first.shape[1]
    z, y = lax.axis_index("shard_0"), lax.axis_index("shard_1")
    g0, g1, g2 = lax.axis_index("grp_0"), lax.axis_index("grp_1"), lax.axis_index("grp_2")
    n1, n2 = sizes[1], sizes[2]
    n_shard, n_grp = planes * 2, sizes[0] * n1 * n2
    shard_me = z * 2 + y
    grp_me = (g0 * n1 + g1) * n2 + g2
    up_z, down_z = lax.rem(z + 1, planes), lax.rem(z + planes - 1, planes)
    own = pl.ds(pl.multiple_of(y * nb, 16), nb)
    other = pl.ds(pl.multiple_of((1 - y) * nb, 16), nb)

    def lanes(c, base=0):
        return pl.ds(pl.multiple_of(base + c * LANES, LANES), LANES)

    def shard_id(p):
        return {"shard_0": p // 2, "shard_1": lax.rem(p, 2)}

    def grp_id(p):
        return {"grp_0": p // (n1 * n2), "grp_1": lax.rem(p // n2, n1), "grp_2": lax.rem(p, n2)}

    def bottom(s, c):
        return low(s, c, chunks)

    def at_hop(h, body):
        s = z + h
        pl.when((s < planes) & (z >= bottom(s, 0)))(lambda: body(s, 0))

        @pl.when(h > 0)
        def _():
            t = lax.rem(z - h + planes, planes)
            pl.when((t > z) & (z < bottom(t, 0)))(lambda: body(t, 1))

    def load(s):
        columns = pl.ds(pl.multiple_of(s * 2 * nb, 128), 2 * nb)
        return pltpu.make_async_copy(qr_hbm.at[:, columns], qr.at[s, own], load_sem.at[s])

    load_ql = pltpu.make_async_copy(ql_hbm, ql, load_sem.at[planes])
    mine_half = pl.ds(pl.multiple_of(y * half, LANES), half)
    swap_half = pl.ds(pl.multiple_of((1 - y) * half, LANES), half)
    load_mine = pltpu.make_async_copy(g_ref.at[:, mine_half], gt.at[z, own], load_sem.at[planes + 1])
    load_swap = pltpu.make_async_copy(g_ref.at[:, swap_half], swapped, load_sem.at[planes + 2])
    load_swap.start()
    load_mine.start()
    loop(0, HOPS + 1, lambda h: at_hop(h, lambda s, k: load(s).start()))
    load_ql.start()

    barrier = pltpu.get_barrier_semaphore()

    def greet(semaphore, ids):
        for peer in ids:
            pl.semaphore_signal(semaphore, inc=1, device_id=peer, device_id_type=MESH)

    x_ids = [{"grp_1": lax.rem(g1 + k, n1)} for k in (1, n1 - 1)] if n1 > 1 else []
    y_ids = [{"shard_1": 1 - y}] + ([{"grp_0": 1 - g0, "shard_1": 1 - y}] if sizes[0] > 1 else [])
    core_ids = [{"grp_2": 1 - g2}] if n2 > 1 else []
    z_ids = [{"shard_0": to, "shard_1": line} for to in (up_z, down_z) for line in (y, 1 - y)]
    greet(barrier, y_ids + z_ids + x_ids + core_ids)
    load_swap.wait()
    load_mine.wait()
    pl.semaphore_wait(barrier, len(y_ids) + len(z_ids) + len(x_ids) + len(core_ids))

    chain = [y_ids, x_ids, x_ids, core_ids]

    def pass_on(k):
        if k > 0:
            pl.semaphore_wait(chain_sem.at[k - 1], len(chain[k - 1])) if chain[k - 1] else None
        if k < len(chain):
            greet(chain_sem.at[k], chain[k])

    pass_on(0)

    def remote(src, dst, send, recv, to_z, to_y):
        return pltpu.make_async_remote_copy(
            src_ref=src,
            dst_ref=dst,
            send_sem=send,
            recv_sem=recv,
            device_id={"shard_0": to_z, "shard_1": to_y},
            device_id_type=MESH,
        )

    def swap(c):
        return remote(swapped.at[:, lanes(c)], gt.at[z, own, lanes(c)], swap_send.at[c], swap_recv.at[c], z, 1 - y)

    def factor(s):
        ref = qr.at[s, own]
        return remote(ref, ref, factor_send.at[s], factor_recv.at[s], z, 1 - y)

    def down(c, s):
        ref = gt.at[s, :, lanes(c)]
        return remote(ref, ref, down_send.at[c, s], gather_recv.at[c, s], down_z, y)

    def up(c, s):
        ref = gt.at[s, :, lanes(c)]
        return remote(ref, ref, up_send.at[c, s], gather_recv.at[c, s], up_z, y)

    def back(c, s, src):
        rising = (z < s) & (z >= bottom(s, c))
        parent = jnp.where(rising, up_z, down_z)
        return remote(src, held.at[c, s], back_send.at[c, s], back_recv.at[c, s], parent, y)

    def last(c, way, k, src):
        to_z = (up_z, down_z)[way]
        send, recv = last_send.at[way, k, c], landed_recv.at[way, y, c]
        return remote(src, landed.at[way, y, c], send, recv, to_z, y if k == 0 else 1 - y)

    def start_last(c, way, ref):
        last(c, way, 0, ref.at[own]).start()
        last(c, way, 1, ref.at[other]).start()

    def final(c):
        return remote(leaving.at[c], coming.at[c], final_send.at[c], final_recv.at[c], z, 1 - y)

    def goes_down(s):
        return (z <= s) & (z - 1 >= bottom(s, 0))

    def goes_up(s):
        return ((z >= s) & (bottom(s, 0) > 0)) | ((z < s) & (z + 1 < bottom(s, 0)))

    def got_back(c, s):
        remote(held.at[c, s], held.at[c, s], back_send.at[0, 0], back_recv.at[c, s], up_z, y).wait_recv()

    def relayed(s):
        return (z == 0) & ((s == 4) | (s == 5))

    def relays(k):
        return (z == 7) & (k >= 0)

    def relay_slot(s):
        return jnp.where((z == 0) & (s == 4), 1, 0)

    def relay_first(s, k):
        via = jnp.where(z == 0, down_z, up_z)
        return remote(qr.at[s, own], relay_in.at[k], relay_send.at[0, k], relay_recv.at[0, k], via, y)

    def relay_second(k):
        return remote(relay_in.at[k], relay_out.at[k], relay_send.at[1, k], relay_recv.at[1, k], z, 1 - y)

    def relay_third(k):
        s = jnp.where(z == 7, 5 - k, z + 3)
        to = jnp.where(z == 7, up_z, down_z)
        return remote(relay_out.at[k], qr.at[s, other], relay_send.at[2, k], factor_recv.at[s], to, y)

    def start_relay(s, k):
        @pl.when(relayed(s))
        def _():
            load(s).wait()
            relay_first(s, relay_slot(s)).start()

    def send_factor(s, k):
        @pl.when(jnp.logical_not(relayed(s)))
        def _():
            load(s).wait()
            factor(s).start()

    def relay_on(k):
        @pl.when(relays(k))
        def _():
            relay_first(z, k).wait_recv()
            relay_second(k).start()

    def relay_home(k):
        @pl.when(relays(k))
        def _():
            relay_second(k).wait_recv()
            relay_third(k).start()

    def piece(c, way, k, s):
        ref = gt.at[s, own if k == 0 else other, lanes(c)]
        return remote(ref, ref, piece_send.at[way, k, c], piece_recv.at[way, k, c], (down_z, up_z)[way], y)

    def start_pieces(c, k):
        pl.when(goes_down(z))(lambda: piece(c, 0, k, z).start())
        pl.when(goes_up(z))(lambda: piece(c, 1, k, z).start())

    def inject(c):
        swap(c).wait_recv()
        start_pieces(c, 1)

    def gather_hop(h, arrive):
        def chunk(c):
            s = z + h

            @pl.when((s < planes) & (z >= bottom(s, 0)))
            def _():
                arrive(c, 0, s)
                pl.when(goes_down(s))(lambda: down(c, s).start())

            t = lax.rem(z - h + planes, planes)

            @pl.when(((z > t) & (bottom(t, 0) > 0)) | ((z < t) & (z < bottom(t, 0))))
            def _():
                arrive(c, 1, t)
                pl.when(goes_up(t))(lambda: up(c, t).start())

        loop(0, chunks, chunk)

    def arrive_pieces(c, way, s):
        piece(c, way, 0, s).wait_recv()
        piece(c, way, 1, s).wait_recv()

    def arrive_whole(c, way, s):
        down(c, s).wait_recv()

    def turn(s):
        qrt[s] = qr[s].T

    def turned_early(s):
        return (s - z < 3) | (s - z > planes - 3)

    def multiply_own(s, k):
        first_sum[own, :] += jnp.dot(qr[s, own, :], gt[s], preferred_element_type=F32)

    def multiply_other(s, k):
        factor(s).wait_recv()
        pl.when(turned_early(s))(lambda: turn(s))
        first_sum[other, :] += jnp.dot(qr[s, other, :], gt[s], preferred_element_type=F32)

    if n2 > 1:
        @pl.when(g2 == 1)
        def _():
            pl.semaphore_wait(turn_sem, 1)

    def let_go():
        if n2 > 1:
            @pl.when(g2 == 0)
            def _():
                pl.semaphore_signal(turn_sem, inc=1, device_id={"grp_2": 1 - g2}, device_id_type=MESH)

    loop(0, chunks, lambda c: swap(c).start())
    at_hop(0, send_factor)
    loop(HOPS - 1, HOPS + 1, lambda h: at_hop(h, start_relay))
    loop(0, chunks, lambda c: start_pieces(c, 0))
    loop(0, chunks, inject)
    relay_on(0)
    loop(1, HOPS + 1, lambda h: at_hop(h, send_factor))
    pass_on(1)
    first_sum[...] = jnp.zeros_like(first_sum)
    gather_hop(1, arrive_pieces)
    relay_on(1)
    relay_home(0)
    pass_on(2)
    at_hop(0, multiply_own)
    at_hop(1, multiply_own)
    at_hop(0, multiply_other)

    def hop(h):
        gather_hop(h, arrive_whole)
        pl.when(h == 2)(let_go)
        pl.when(h == 2)(lambda: relay_home(1))
        at_hop(h, multiply_own)
        at_hop(h - 1, multiply_other)

    loop(2, HOPS + 1, hop)
    pass_on(3)
    at_hop(HOPS, multiply_other)
    first[...] = first_sum[...].astype(BF16)

    def product(s, k):
        pl.when(jnp.logical_not(turned_early(s)))(lambda: turn(s))
        share[k] = jnp.dot(qrt[s], first[...], preferred_element_type=F32)

    def contribute(c, s, k, send):
        floor = bottom(s, c)
        child = ((z >= floor) & (z - 1 >= floor)) | (z + 1 < floor)

        @pl.when(child)
        def _():
            got_back(c, s)
            part[c, s] = (share[k, :, lanes(c)] + held[c, s].astype(F32)).astype(BF16)

        @pl.when(jnp.logical_not(child))
        def _():
            part[c, s] = share[k, :, lanes(c)].astype(BF16)

        send(c, s, k, part.at[c, s])

    def back_phase(h, send):
        at_hop(h, product)

        def chunk(c):
            at_hop(h, lambda s, k: contribute(c, s, k, send))
            t = z - h

            @pl.when((t >= 0) & (bottom(t, c) > 0))
            def _():
                got_back(c, t)
                send(c, t, 1, held.at[c, t])

        loop(0, chunks, chunk)

    def send_back(c, s, k, ref):
        back(c, s, ref).start()

    def send_last(c, s, k, ref):
        start_last(c, k, ref)

    loop(0, HOPS - 2, lambda i: back_phase(HOPS - i, send_back))

    product(z, 0)
    kept[...] = share[0, own, :]

    def leave(c):
        leaving[c] = share[0, other, lanes(c)]
        final(c).start()

    loop(0, chunks, leave)
    back_phase(2, send_back)
    back_phase(1, send_last)

    def arrived(way, line, c):
        return remote(
            landed.at[way, line, c],
            landed.at[way, line, c],
            last_send.at[0, 0, 0],
            landed_recv.at[way, line, c],
            up_z,
            y,
        )

    def finish(c):
        final(c).wait_recv()

        @pl.when(z > 0)
        def _():
            arrived(0, y, c).wait_recv()
            arrived(0, 1 - y, c).wait_recv()
            kept[:, lanes(c)] += landed[0, y, c].astype(F32)
            coming[c] += landed[0, 1 - y, c].astype(F32)

        @pl.when(bottom(z, c) > 0)
        def _():
            arrived(1, y, c).wait_recv()
            arrived(1, 1 - y, c).wait_recv()
            kept[:, lanes(c)] += landed[1, y, c].astype(F32)
            coming[c] += landed[1, 1 - y, c].astype(F32)

        second[y * chunks + c] = kept[:, lanes(c)].astype(BF16)
        second[(1 - y) * chunks + c] = coming[c].astype(BF16)

    loop(0, chunks, finish)

    load_ql.wait()
    sub = jnp.concatenate([second[c] for c in range(2 * chunks)], axis=1)
    third = lax.dot_general(sub, ql[...], (((1,), (1,)), ((), ())), preferred_element_type=F32).astype(BF16)
    precond[...] = jnp.dot(third, ql[...], preferred_element_type=F32)

    value = precond[...]
    square = value * value
    tile = square[0:8]
    for r in range(8, nb, 8):
        tile = tile + square[r : r + 8]
    total = tile[:, 0:128]
    for k in range(128, value.shape[1], 128):
        total = total + tile[:, k : k + 128]
    mine[...] = jnp.sum(total, axis=0, keepdims=True)

    def exchange(phase, n, me, ident, slots):
        slots[me] = mine[...]

        def make(peer, at):
            return pltpu.make_async_remote_copy(
                src_ref=mine,
                dst_ref=slots.at[at],
                send_sem=ar_send.at[phase, peer],
                recv_sem=ar_recv.at[phase, at],
                device_id=ident(peer),
                device_id_type=MESH,
            )

        loop(1, n, lambda k: make(lax.rem(me + k, n), me).start())

        def wait(k):
            peer = lax.rem(me + k, n)
            make(peer, peer).wait_recv()

        loop(1, n, wait)
        loop(1, n, lambda k: make(lax.rem(me + k, n), me).wait_send())
        total = slots[0]
        for k in range(1, n):
            total = total + slots[k]
        mine[...] = total

    pass_on(4)
    exchange(0, n_shard, shard_me, shard_id, all_shard)
    exchange(1, n_grp, grp_me, grp_id, all_grp)

    rms = jnp.sqrt(jnp.sum(mine[...], keepdims=True) / count + 1e-06)
    scale = jnp.minimum(jnp.float32(1.0), 1.1 / rms)
    out_ref[...] = (precond[...] * scale).astype(BF16)

    def drain(c):
        swap(c).wait_send()
        final(c).wait_send()
        for k in range(2):
            pl.when(goes_down(z))(lambda: piece(c, 0, k, z).wait_send())
            pl.when(goes_up(z))(lambda: piece(c, 1, k, z).wait_send())
            pl.when(z < planes - 1)(lambda: last(c, 0, k, part.at[c, 0, own]).wait_send())
            falls = (z == 0) | (bottom(z - 1, c) > 0)
            pl.when(falls)(lambda: last(c, 1, k, part.at[c, 0, own]).wait_send())

        def each(s):
            pl.when(goes_down(s) & (s != z))(lambda: down(c, s).wait_send())
            pl.when(goes_up(s) & (s != z))(lambda: up(c, s).wait_send())
            comes = (z < s) | ((z > s) & (bottom(s, c) > 0))
            near = (s == z + 1) | (s == down_z)
            pl.when(comes & jnp.logical_not(near))(lambda: back(c, s, part.at[c, s]).wait_send())

        loop(0, planes, each)

    loop(0, chunks, drain)

    def drain_factor(s):
        pl.when(relayed(s))(lambda: relay_first(s, relay_slot(s)).wait_send())
        pl.when(jnp.logical_not(relayed(s)))(lambda: factor(s).wait_send())

    def drain_relay(k):
        @pl.when(relays(k))
        def _():
            relay_second(k).wait_send()
            relay_third(k).wait_send()

    loop(z, planes, drain_factor)
    loop(0, 2, drain_relay)


def body(sizes, gradients, left_factor, right_factor):
    rows, nb = gradients.shape[1:]
    half = rows // 2
    chunks = half // LANES
    planes = PLANES
    n_shard, n_grp = 2 * planes, sizes[0] * sizes[1] * sizes[2]
    count = gradients.shape[0] * n_grp * rows * nb * n_shard
    dma = pltpu.SemaphoreType.DMA
    turned = pl.pallas_call(
        functools.partial(kernel, count, sizes),
        out_shape=jax.ShapeDtypeStruct((nb, rows), BF16),
        in_specs=[
            pl.BlockSpec(memory_space=pl.ANY),
            pl.BlockSpec(memory_space=pl.ANY),
            pl.BlockSpec(memory_space=pl.ANY),
        ],
        out_specs=pl.BlockSpec(memory_space=pltpu.VMEM),
        scratch_shapes=[
            pltpu.VMEM((planes, 2 * nb, half), BF16),
            pltpu.VMEM((chunks, planes, 2 * nb, LANES), BF16),
            pltpu.VMEM((chunks, planes, 2 * nb, LANES), BF16),
            pltpu.VMEM((planes, 2 * nb, 2 * nb), BF16),
            pltpu.VMEM((planes, 2 * nb, 2 * nb), BF16),
            pltpu.VMEM((rows, rows), BF16),
            pltpu.VMEM((2 * nb, half), BF16),
            pltpu.VMEM((2 * nb, half), F32),
            pltpu.VMEM((2, 2 * nb, half), F32),
            pltpu.VMEM((2 * chunks, nb, LANES), BF16),
            pltpu.VMEM((chunks, nb, LANES), F32),
            pltpu.VMEM((chunks, nb, LANES), F32),
            pltpu.VMEM((nb, half), F32),
            pltpu.VMEM((2, 2, chunks, nb, LANES), BF16),
            pltpu.VMEM((nb, half), BF16),
            pltpu.VMEM((2, nb, 2 * nb), BF16),
            pltpu.VMEM((2, nb, 2 * nb), BF16),
            pltpu.VMEM((nb, rows), F32),
            pltpu.VMEM((1, 128), F32),
            pltpu.VMEM((n_shard, 1, 128), F32),
            pltpu.VMEM((n_grp, 1, 128), F32),
            dma((chunks, planes)),
            dma((chunks, planes)),
            dma((chunks, planes)),
            dma((2, 2, chunks)),
            dma((2, 2, chunks)),
            dma((chunks, planes)),
            dma((chunks, planes)),
            dma((2, 2, chunks)),
            dma((2, 2, chunks)),
            dma((chunks,)),
            dma((chunks,)),
            dma((planes,)),
            dma((planes,)),
            dma((3, 2)),
            dma((2, 2)),
            dma((chunks,)),
            dma((chunks,)),
            dma((planes + 3,)),
            pltpu.SemaphoreType.REGULAR((4,)),
            pltpu.SemaphoreType.REGULAR,
            dma((2, max(n_shard, n_grp))),
            dma((2, max(n_shard, n_grp))),
        ],
        compiler_params=pltpu.CompilerParams(
            collective_id=0, has_side_effects=True, vmem_limit_bytes=55500000
        ),
        name="precondition",
    )(gradients[0].T, right_factor[0], left_factor[0])
    return turned.T[None]


def split_mesh(devices, sizes):
    return Mesh(devices.reshape(*sizes, PLANES, 2), GRP + SHARD)


def program(split, sizes):
    in_specs = (P(GRP, None, SHARD), P(GRP, None, None), P(GRP, SHARD, None))
    return jax.shard_map(
        functools.partial(body, sizes), mesh=split, in_specs=in_specs, out_specs=P(GRP, None, SHARD), check_vma=False
    )


def solution(mesh):
    sizes = (2, 4, 2)
    return program(split_mesh(mesh.devices, sizes), sizes)
```
